32 devices in a mesh: grp: 2 (over y), ep: 8 (over z, x), tp: 2 (over core).
Axes of the slice: x: 2, y: 2, z: 4, core: 2. Of those that a mesh axis runs over, the one named last changes fastest.
Arguments:
- queries: bfloat16 [1024, 16, 576], P(('grp', 'ep'), 'tp'), parts along dimension 0, may hold values from -450 to 450
- latent_cache: bfloat16 [48, 512, 576], P(('grp', 'ep'), 'tp'), parts along dimension 0, may hold values from -6 to 6
- residual: bfloat16 [1024, 2048], P(('grp', 'ep')), parts along dimension 0, may hold values from -8 to 8
- token_request: int32 [1024], P(('grp', 'ep')), parts along dimension 0, may hold values from 0 to 2, as said below
- token_visible: int32 [1024], P(('grp', 'ep')), parts along dimension 0, may hold values from 1 to 512, as said below
- value_proj: bfloat16 [16, 512, 128], P('tp', 'ep'), may hold values from -0.25 to 0.25
- out_proj: bfloat16 [2048, 2048], P('tp', 'ep'), may hold values from -0.125 to 0.125
- norm_gain: float32 [2048], replicated, may hold values from 0.1 to 1.9
- router: bfloat16 [2048, 64], replicated, may hold values from -0.0390625 to 0.0390625
- expert_ids: int32 [1024, 6], P(('grp', 'ep')), parts along dimension 0, may hold values from 0 to 63, all different within a row; in each aligned block of 64 rows (0 to 63, 64 to 127, ...) at most 8 rows name the same one
- gate_weight: bfloat16 [128, 2048, 384], P('ep', None, 'tp'), may hold values from -0.125 to 0.125
- up_weight: bfloat16 [128, 2048, 384], P('ep', None, 'tp'), may hold values from -0.125 to 0.125
- down_weight: bfloat16 [128, 384, 2048], P('ep', 'tp'), may hold values from -0.21875 to 0.21875
Outputs:
- hidden: bfloat16 [1024, 2048], P(('grp', 'ep'), 'tp'), parts along dimension 0
- expert_out: bfloat16 [1024, 2048], P(('grp', 'ep'), 'tp'), parts along dimension 0
The draws below stay inside these ranges and needn't reach their ends.
There are 2 independent parts, one for each index of `grp`. The reference program is written for one: setup_inputs(seed, part) draws one part's arguments, and reference() takes and returns one part's arrays. A program takes and returns all parts, laid end to end along the dimension named above; an argument that names none is the same for every part. Nothing has to cross between parts.
Inputs may be any that keep to these rules, and one draw needn't show every extreme that they name: `token_request`: in each ep block, 62 tokens belong to request 0, a prefill span, and each other request has exactly one token; the tokens' order in the block is arbitrary. `token_visible`: the span's tokens read consecutive counts s + 1 to s + 62; 512 is reached in every draw. `expert_ids`: each row names 6 different experts; among the 64 tokens of one ep index no expert is named by more than 8 tokens, and this bound is reached.
All inputs are finite; a program needn't handle non-finite values.
Results may differ from the reference program's by a relative error of at most 0.018.
Values may be sent and summed in bfloat16 or wider, within the bound.
A program may use at most 128 MiB of HBM per device.

```python
import math
import jax
import jax.numpy as jnp
import numpy as np
from jax import lax

D = 2048
HEADS = 16
LATENT = 512
ROPE = 64
VDIM = 128
EXPERTS = 64
TOPK = 6
EXP_HIDDEN = 768
GROUPS = 2
TOK_DEV = 64
REQ_DEV = 3
CACHE_LEN = 512
CAP = 8
PIECES = 128
TOKENS = 512
REQS = 24
N_EP = 8
N_TP = 2


def request_layout(key):
    blocks = TOKENS // TOK_DEV
    prefill = TOK_DEV - REQ_DEV + 1
    streams = jax.random.split(jax.random.fold_in(key, 101), blocks)

    def one_block(stream, block_index):
        first, second, third = jax.random.split(stream, 3)
        ordering = jax.random.permutation(first, TOK_DEV).astype(jnp.int32)
        span_start = jax.random.randint(second, (), 0, CACHE_LEN - prefill + 1)
        lengths = jax.random.randint(third, (REQ_DEV - 1,), 1, CACHE_LEN + 1)
        lengths = jnp.where((block_index == 0) & (jnp.arange(REQ_DEV - 1) == 0), CACHE_LEN, lengths)
        in_span = ordering < prefill
        request = jnp.where(in_span, 0, ordering - prefill + 1)
        decode_index = jnp.clip(ordering - prefill, 0, REQ_DEV - 2)
        visible = jnp.where(in_span, span_start + ordering + 1, lengths[decode_index])
        return (request.astype(jnp.int32), visible.astype(jnp.int32))
    request, visible = jax.vmap(one_block)(streams, jnp.arange(blocks))
    return (request.reshape(TOKENS), visible.reshape(TOKENS))


def draw_token_request(key, part):
    return request_layout(key)[0]


def draw_token_visible(key, part):
    return request_layout(key)[1]


def cache_rope(key):
    return jnp.clip(jax.random.normal(jax.random.fold_in(key, 202), (REQS, CACHE_LEN, ROPE)), -4.0, 4.0)


def draw_latent_cache(key, part):
    latent = jnp.clip(jax.random.normal(jax.random.fold_in(key, 201), (REQS, CACHE_LEN, LATENT)), -4.0, 4.0)
    return jnp.concatenate([latent, cache_rope(key)], axis=2).astype(jnp.bfloat16)


def draw_queries(key, part):
    shape = (TOKENS, HEADS, LATENT + ROPE)
    values = 0.6 * jnp.clip(jax.random.normal(jax.random.fold_in(key, 301), shape), -4.0, 4.0)
    return values.astype(jnp.bfloat16)


def draw_residual(key, part):
    scales = jnp.exp(jax.random.uniform(jax.random.fold_in(key, 401), (TOKENS, 1), minval=jnp.log(0.2), maxval=jnp.log(2.0)))
    noise = jnp.clip(jax.random.normal(jax.random.fold_in(key, 402), (TOKENS, D)), -4.0, 4.0)
    return (scales * noise).astype(jnp.bfloat16)


def steps_of(own_key, extent, pieces, least, top_value):
    def one(dim, shards_of):
        heights = jax.random.uniform(jax.random.fold_in(jax.random.fold_in(own_key, 6), dim), (shards_of,), jnp.float32, least / len(pieces), top_value / len(pieces))
        return jnp.repeat(jnp.exp(heights), extent[dim] // shards_of).reshape((-1,) + (1,) * (len(extent) - dim - 1))

    level = one(*pieces[0])
    for cut in pieces[1:]:
        level = level * one(*cut)
    return level


def deal_out(stream_key, own, number, rows, count, top, most, skew):
    order = jax.random.permutation(stream_key, count)
    heavy_load, usual = portions_of(count, rows * top, most, skew, True), portions_of(count, rows * top, most, skew, False)
    places = jnp.arange(count)

    def named(tallies, offset_by):
        used = int((tallies > 0).sum())
        fixed = max(1, used // 4)
        moved = fixed + (places - fixed + offset_by * (used - fixed)) % max(1, count - fixed)
        return jnp.zeros((count,), jnp.int32).at[order[jnp.where(places < fixed, places, moved)]].set(jnp.asarray(tallies, jnp.int32))

    tallies = jnp.where(number % 4 == 0, named(heavy_load, number // 4), named(usual, number - number // 4 - 1))
    mixed = jax.random.permutation(jax.random.fold_in(own, 3), count)
    source_of, taker = mixed[0:count // 2 * 2:2], mixed[1:count // 2 * 2:2]
    margin = jnp.minimum(tallies[source_of] - 1, most - tallies[taker]) // 2
    margin = jnp.where((source_of == order[0]) | (taker == order[0]) | (tallies[taker] == 0), 0, jnp.maximum(margin, 0))
    moved = jax.random.randint(jax.random.fold_in(own, 4), (count // 2,), 0, 1 << 20) % (margin + 1)
    tallies = tallies.at[source_of].add(-moved).at[taker].add(moved)
    items = jnp.searchsorted(jnp.cumsum(tallies), jnp.arange(rows * top), side="right").astype(jnp.int32)
    grid = items.reshape(top, rows).T
    grid = grid[jax.random.permutation(jax.random.fold_in(own, 1), rows)]
    offset_by = jax.random.randint(jax.random.fold_in(own, 2), (rows, 1), 0, top)
    return jnp.take_along_axis(grid, (jnp.arange(top)[None, :] + offset_by) % top, axis=1)


def portions_of(amount, total, reach, lean, full):
    loads = [(1 << 20) // math.isqrt(grade ** lean) + 1 for grade in range(1, amount + 1)]
    largest = reach if full else min(reach, max(-(-total // amount), total * loads[0] // sum(loads)))
    least = 1 if total - largest >= amount - 1 else 0
    given, surplus = [largest] + [least] * (amount - 1), total - largest - least * (amount - 1)
    while surplus > 0:
        movable = [i for i in range(1, amount) if given[i] < largest] or [i for i in range(1, amount) if given[i] < reach]
        mass, remaining = sum([loads[i] for i in movable]), surplus
        for i in movable:
            more = min(reach - given[i], max(1, remaining * loads[i] // mass), surplus)
            given[i] = given[i] + more
            surplus = surplus - more
    return np.array(given)


def bell_draw(stream_key, shape, width, most, cuts=(), held_as=jnp.bfloat16):
    gain = steps_of(stream_key, shape, cuts, -0.22, 0.18) if cuts else 1.0
    array = jax.random.normal(stream_key, shape, jnp.float32) * width * gain
    return jnp.minimum(jnp.maximum(array, -most), most).astype(held_as)


def setup_inputs(seed: int = 0, part: int = 0) -> dict:
    key_of = jax.random.split(jax.random.key(seed), 14)
    part_keys = jax.random.split(jax.random.fold_in(key_of[13], part), 14)
    queries = draw_queries(jax.random.fold_in(jax.random.fold_in(key_of[13], part), 71), part)
    latent_cache = draw_latent_cache(jax.random.fold_in(jax.random.fold_in(key_of[13], part), 71), part)
    residual = draw_residual(jax.random.fold_in(jax.random.fold_in(key_of[13], part), 71), part)
    token_request = draw_token_request(jax.random.fold_in(jax.random.fold_in(key_of[13], part), 71), part)
    token_visible = draw_token_visible(jax.random.fold_in(jax.random.fold_in(key_of[13], part), 71), part)
    value_proj = bell_draw(key_of[5], (HEADS, LATENT, VDIM), LATENT ** -0.5, 0.25, ((0, 2), (1, 8)))
    out_proj = bell_draw(key_of[6], (HEADS * VDIM, D), (HEADS * VDIM) ** -0.5, 0.125, ((0, 2), (1, 8)))
    norm_gain = jnp.clip(1.0 + 0.18 * jax.random.normal(key_of[7], (D,), jnp.float32), 0.1, 1.9)
    router = bell_draw(key_of[8], (D, EXPERTS), (12 * D) ** -0.5, 0.0390625)
    expert_ids_keys = jax.random.split(jax.random.fold_in(part_keys[9], 1), TOKENS // TOK_DEV)
    expert_ids_turns = jax.random.permutation(jax.random.fold_in(part_keys[9], 3), TOKENS // TOK_DEV)
    expert_ids = jax.vmap(lambda own, number: deal_out(jax.random.fold_in(part_keys[9], 2), own, number, TOK_DEV, EXPERTS, TOPK, CAP, 2))(expert_ids_keys, expert_ids_turns).reshape((TOKENS, TOPK))
    gate_weight = bell_draw(key_of[10], (PIECES, D, EXP_HIDDEN // GROUPS), D ** -0.5, 0.125, ((0, 8), (2, 2)))
    up_weight = bell_draw(key_of[11], (PIECES, D, EXP_HIDDEN // GROUPS), D ** -0.5, 0.125, ((0, 8), (2, 2)))
    down_weight = bell_draw(key_of[12], (PIECES, EXP_HIDDEN // GROUPS, D), EXP_HIDDEN ** -0.5, 0.21875, ((0, 8), (1, 2)))
    return {"queries": queries, "latent_cache": latent_cache, "residual": residual, "token_request": token_request, "token_visible": token_visible, "value_proj": value_proj, "out_proj": out_proj, "norm_gain": norm_gain, "router": router, "expert_ids": expert_ids, "gate_weight": gate_weight, "up_weight": up_weight, "down_weight": down_weight}


score_scale = 192.0 ** (-0.5)
epsilon = 1e-06

def attend_block(arrays):
    queries, block_rows, token_request, token_visible = arrays
    per_request = block_rows.shape[1]
    flat_rows = block_rows.reshape(-1, block_rows.shape[2]).astype(jnp.float32)
    scores = jnp.einsum('thc,kc->thk', queries.astype(jnp.float32), flat_rows) * score_scale
    column = jnp.arange(flat_rows.shape[0], dtype=jnp.int32)
    owner_id = column // per_request
    position = column % per_request
    allowed = (owner_id[None, :] == token_request[:, None]) & (position[None, :] < token_visible[:, None])
    scores = jnp.where(allowed[:, None, :], scores, -jnp.inf)
    row_peak = lax.optimization_barrier(jnp.max(scores, axis=2, keepdims=True))
    rounded = lax.optimization_barrier(jnp.exp(scores - row_peak).astype(jnp.bfloat16))
    weights = rounded.astype(jnp.float32)
    totals = lax.optimization_barrier(jnp.sum(weights, axis=2, keepdims=True))
    summed = jnp.einsum('thk,kc->thc', weights, flat_rows[:, :LATENT])
    return (summed / totals).astype(jnp.bfloat16)

def reference(queries, latent_cache, residual, token_request, token_visible, value_proj, out_proj, norm_gain, router, expert_ids, gate_weight, up_weight, down_weight):
    blocks = TOKENS // TOK_DEV
    context = lax.map(attend_block, (queries.reshape(blocks, TOK_DEV, HEADS, LATENT + ROPE), latent_cache.reshape(blocks, REQ_DEV, CACHE_LEN, LATENT + ROPE), token_request.reshape(blocks, TOK_DEV), token_visible.reshape(blocks, TOK_DEV)))
    context = context.reshape(TOKENS, HEADS, LATENT)
    heads_out = jnp.einsum('thl,hlv->thv', context.astype(jnp.float32), value_proj.astype(jnp.float32)).astype(jnp.bfloat16)
    heads_out = heads_out.reshape(TOKENS, HEADS * VDIM)
    attention = jnp.dot(heads_out, out_proj, preferred_element_type=jnp.float32)
    hidden = (residual.astype(jnp.float32) + attention).astype(jnp.bfloat16)
    hidden_wide = hidden.astype(jnp.float32)
    normed = (hidden_wide * lax.rsqrt(lax.optimization_barrier(jnp.mean(hidden_wide * hidden_wide, axis=1, keepdims=True)) + epsilon) * norm_gain).astype(jnp.bfloat16)
    logits = jnp.dot(normed, router, preferred_element_type=jnp.float32)
    gate_share = jax.nn.softmax(jnp.take_along_axis(logits, expert_ids, axis=1), axis=1).astype(jnp.bfloat16)
    flat_ids = expert_ids.reshape(-1)
    flat_share = gate_share.reshape(-1).astype(jnp.float32)
    bound = N_EP * CAP
    part_width = EXP_HIDDEN // (GROUPS * N_TP)

    def piece_step(running, piece_index):
        expert = piece_index // GROUPS
        hit_mask = flat_ids == expert
        hits = jnp.nonzero(hit_mask, size=bound, fill_value=0)[0].astype(jnp.int32)
        live = jnp.arange(bound, dtype=jnp.int32) < jnp.sum(hit_mask.astype(jnp.int32))
        token_rows = hits // TOPK
        picked = normed[token_rows]
        gate_vals = jnp.dot(picked, gate_weight[piece_index], preferred_element_type=jnp.float32)
        up_vals = jnp.dot(picked, up_weight[piece_index], preferred_element_type=jnp.float32)
        activated = (jax.nn.silu(gate_vals) * up_vals).astype(jnp.bfloat16)
        combined = jnp.zeros((bound, D), jnp.float32)
        for half_index in range(N_TP):
            lower = half_index * part_width
            piece_out = jnp.dot(activated[:, lower:lower + part_width], down_weight[piece_index, lower:lower + part_width], preferred_element_type=jnp.float32).astype(jnp.bfloat16)
            combined = combined + piece_out.astype(jnp.float32)
        scaled = combined * jnp.where(live, flat_share[hits], 0.0)[:, None]
        return (running.at[token_rows].add(scaled), None)
    routed, _ = lax.scan(piece_step, jnp.zeros((TOKENS, D), jnp.float32), jnp.arange(PIECES, dtype=jnp.int32))
    return (hidden, routed.astype(jnp.bfloat16))
```

```python
import functools

import jax
import jax.numpy as jnp
from jax import lax
from jax.experimental import pallas as pl
from jax.experimental.pallas import tpu as pltpu
from jax.sharding import PartitionSpec as P

LATENT = 512
VDIM = 128
EXPERTS = 64
TOPK = 6
GROUPS = 2
CAP = 8
PIECES = 128
MESH = pl.DeviceIdType.MESH


score_scale = 192.0 ** (-0.5)
epsilon = 1e-06


def masked_scores(queries, block_rows, token_request, token_visible):
    per_request = block_rows.shape[1]
    flat_rows = block_rows.reshape(-1, block_rows.shape[2])
    scores = (
        jnp.einsum("thc,kc->thk", queries, flat_rows, preferred_element_type=jnp.float32)
        * score_scale
    )
    column = jnp.arange(flat_rows.shape[0], dtype=jnp.int32)
    owner_id = column // per_request
    position = column % per_request
    allowed = (owner_id[None, :] == token_request[:, None]) & (
        position[None, :] < token_visible[:, None]
    )
    return (jnp.where(allowed[:, None, :], scores, -jnp.inf), flat_rows)


def weighted_rows(scores, row_peak, flat_rows):
    weights = jnp.exp(scores - row_peak[:, :, None]).astype(jnp.bfloat16)
    totals = jnp.sum(weights.astype(jnp.float32), axis=2)
    summed = jnp.einsum(
        "thk,kc->thc", weights, flat_rows[:, :LATENT], preferred_element_type=jnp.float32
    )
    return (summed, totals)


def expert_block(arrived, gate_weight, up_weight, down_weight):
    gate_vals = jnp.einsum("prd,pdf->prf", arrived, gate_weight, preferred_element_type=jnp.float32)
    up_vals = jnp.einsum("prd,pdf->prf", arrived, up_weight, preferred_element_type=jnp.float32)
    activated = (jax.nn.silu(gate_vals) * up_vals).astype(jnp.bfloat16)
    return jnp.einsum(
        "prf,pfd->prd", activated, down_weight, preferred_element_type=jnp.float32
    ).astype(jnp.bfloat16)


def body(
    queries,
    latent_cache,
    residual,
    token_request,
    token_visible,
    value_proj,
    out_proj,
    norm_gain,
    router,
    expert_ids,
    gate_weight,
    up_weight,
    down_weight,
):
    all_rows = lax.all_gather(latent_cache, "tp", axis=1, tiled=True)
    scores, flat_rows = masked_scores(queries, all_rows, token_request, token_visible)
    summed, totals = weighted_rows(scores, jnp.max(scores, axis=2), flat_rows)
    context = (summed / totals[:, :, None]).astype(jnp.bfloat16)
    tokens_here = context.shape[0]
    heads_here = context.shape[1]
    head_values = jnp.einsum(
        "thl,hlv->thv",
        context,
        lax.all_gather(value_proj, "ep", axis=1, tiled=True),
        preferred_element_type=jnp.float32,
    )
    heads_out = head_values.astype(jnp.bfloat16).reshape(tokens_here, heads_here * VDIM)
    column_block = jnp.dot(
        lax.all_gather(heads_out, "ep", axis=0, tiled=True),
        out_proj,
        preferred_element_type=jnp.float32,
    )
    attention_part = lax.all_to_all(column_block, "ep", split_axis=0, concat_axis=1, tiled=True)
    attention = lax.psum(attention_part, "tp")
    hidden = (residual.astype(jnp.float32) + attention).astype(jnp.bfloat16)
    hidden_wide = hidden.astype(jnp.float32)
    normed = (
        hidden_wide
        * lax.rsqrt(jnp.mean(hidden_wide * hidden_wide, axis=1, keepdims=True) + epsilon)
        * norm_gain
    ).astype(jnp.bfloat16)
    logits = jnp.dot(normed, router, preferred_element_type=jnp.float32)
    gate_share = jax.nn.softmax(jnp.take_along_axis(logits, expert_ids, axis=1), axis=1).astype(
        jnp.bfloat16
    )
    flat_ids = expert_ids.reshape(-1)
    position_id = jnp.arange(flat_ids.shape[0], dtype=jnp.int32)
    earlier = (flat_ids[:, None] == flat_ids[None, :]) & (
        position_id[None, :] < position_id[:, None]
    )
    slot_ids = (flat_ids * CAP + jnp.sum(earlier.astype(jnp.int32), axis=1)).reshape(
        tokens_here, TOPK
    )
    targets = jnp.arange(EXPERTS * CAP, dtype=jnp.int32)
    matches = slot_ids[:, :, None] == targets[None, None, :]
    picker = jnp.any(matches, axis=1).T.astype(jnp.bfloat16)
    model_width = normed.shape[1]
    mixing = jnp.sum(
        jnp.where(matches, gate_share[:, :, None], jnp.zeros((), jnp.bfloat16)), axis=1
    )
    mixing = jnp.broadcast_to(
        mixing.reshape(tokens_here, EXPERTS, 1, CAP), (tokens_here, EXPERTS, GROUPS, CAP)
    ).reshape(tokens_here, PIECES * CAP)
    core_count = lax.axis_size("tp")
    half_width = model_width // core_count
    core_start = lax.axis_index("tp") * half_width
    outgoing = jnp.dot(picker, normed, preferred_element_type=jnp.float32).astype(jnp.bfloat16)
    outgoing = jnp.broadcast_to(
        outgoing.reshape(EXPERTS, 1, CAP, model_width), (EXPERTS, GROUPS, CAP, model_width)
    ).reshape(PIECES, CAP, model_width)
    arrived = lax.all_to_all(outgoing, "ep", split_axis=0, concat_axis=1, tiled=True)
    partial_out = expert_block(arrived, gate_weight, up_weight, down_weight)
    returned = lax.all_to_all(partial_out, "ep", split_axis=1, concat_axis=0, tiled=True)
    routed = jnp.dot(
        mixing, returned.reshape(PIECES * CAP, model_width), preferred_element_type=jnp.float32
    )
    expert_out = lax.psum_scatter(
        routed.astype(jnp.bfloat16), "tp", scatter_dimension=1, tiled=True
    )
    hidden_part = lax.dynamic_slice_in_dim(hidden, core_start, half_width, 1)
    return (hidden_part, expert_out)


def ring_position(index, count):
    half = lax.div(index, 2)
    return half + lax.rem(index, 2) * (count - 1 - 2 * half)


def ring_index(place, count):
    place = lax.rem(place + count, count)
    upper = lax.div(place, count // 2)
    return 2 * place + upper * (2 * count - 1 - 4 * place)


def greet(count):
    me = lax.axis_index("ep")
    core = lax.axis_index("tp")
    barrier = pltpu.get_barrier_semaphore()
    for step in range(1, count):
        pl.semaphore_signal(
            barrier, inc=1, device_id={"ep": lax.rem(me + step, count)}, device_id_type=MESH
        )
    pl.semaphore_signal(barrier, inc=1, device_id={"tp": 1 - core}, device_id_type=MESH)
    pl.semaphore_wait(barrier, count)


def remote(src, dst, send_sem, recv_sem, where):
    return pltpu.make_async_remote_copy(
        src_ref=src,
        dst_ref=dst,
        send_sem=send_sem,
        recv_sem=recv_sem,
        device_id=where,
        device_id_type=MESH,
    )


def copy_here(src, dst, sem):
    copy = pltpu.make_async_copy(src, dst, sem)
    copy.start()
    return copy


class Ring:
    def __init__(self, count, own, slot, send_sem, recv_sem):
        self.count = count
        self.place = ring_position(lax.axis_index("ep"), count)
        self.far = count // 2
        self.near = count - 1 - self.far
        self.to = (ring_index(self.place + 1, count), ring_index(self.place - 1, count))
        self.own, self.slot = own, slot
        self.send_sem, self.recv_sem = send_sem, recv_sem
        self.hops = {}

    def reach(self, way, part):
        return self.far if way == part else self.near

    def origin(self, way, step):
        return ring_index(self.place - step if way == 0 else self.place + step, self.count)

    def hop(self, way, step, part):
        if step > self.reach(way, part):
            return
        block = self.origin(way, step - 1)
        self.hops[way, step, part] = remote(
            self.own(part) if step == 1 else self.slot(block, part),
            self.slot(block, part),
            self.send_sem.at[way, step - 1, part],
            self.recv_sem.at[way, step - 1, part],
            {"ep": self.to[way]},
        )
        self.hops[way, step, part].start()

    def launch(self):
        for turn in range(2):
            for way in range(2):
                self.hop(way, 1, (way + turn) % 2)

    def relay(self, step):
        for turn in range(2):
            for way in range(2):
                part = (way + turn) % 2
                if step <= self.reach(way, part):
                    self.hops[way, step, part].wait_recv()
                    self.hop(way, step + 1, part)

    def finish(self):
        for copy in self.hops.values():
            copy.wait_send()


def number_of(offset, count):
    far = count // 2
    offset = offset % count
    if offset > far:
        offset -= count
    if offset == 0:
        return 0
    if offset == far:
        return count - 1
    return -2 * offset - 1 if offset < 0 else 2 * offset


def offset_of(number, count):
    if number == count - 1:
        return count // 2
    step = (number + 1) // 2
    return -step if number % 2 else step


class Pieces:
    def __init__(self, count, held, ring_send, ring_recv, side_send, side_recv):
        self.count = count
        self.place = ring_position(lax.axis_index("ep"), count)
        self.core = lax.axis_index("tp")
        self.far = count // 2
        self.near = count - 1 - self.far
        self.to = (ring_index(self.place + 1, count), ring_index(self.place - 1, count))
        self.held = held
        self.sems = (ring_send, ring_recv, side_send, side_recv)
        self.hops, self.sides = {}, {}

    def piece(self, offset, number):
        block = ring_index(self.place + offset + offset_of(number, self.count), self.count)
        return self.held.at[block, ring_index(self.place + offset, self.count), self.core]

    def reach(self, way, number):
        return self.far if number % 2 == way else self.near

    def hop(self, way, step, number):
        if step > self.reach(way, number):
            return
        ref = self.piece(-(step - 1) if way == 0 else step - 1, number)
        copy = remote(
            ref, ref, self.sems[0].at[number, way, step - 1], self.sems[1].at[number, way, step - 1],
            {"ep": self.to[way]},
        )
        copy.start()
        self.hops[way, step, number] = copy

    def side(self, offset, number):
        ref = self.piece(offset, number)
        where = offset % self.count
        copy = remote(
            ref, ref, self.sems[2].at[number, where], self.sems[3].at[number, where],
            {"tp": 1 - self.core},
        )
        copy.start()
        self.sides[where, number] = copy

    def launch(self, number):
        for turn in range(2):
            self.hop((number + turn) % 2, 1, number)
        self.side(0, number)

    def relay(self, step, number):
        for turn in range(2):
            way = (number + turn) % 2
            if step <= self.reach(way, number):
                self.hops[way, step, number].wait_recv()
                self.hop(way, step + 1, number)
                self.side(-step if way == 0 else step, number)

    def settle(self, offset):
        for other in range(self.count):
            self.sides[other, number_of(offset - other, self.count)].wait_recv()

    def finish(self):
        for copy in list(self.hops.values()) + list(self.sides.values()):
            copy.wait_send()


def group_of(step, count):
    far = count // 2
    if step == 0:
        return [0]
    if step == far:
        return [count - 1]
    return [2 * step - 1, 2 * step]


ROWS = 256


def layer_kernel(
    count, meta_ref, gain_ref, queries_hbm, cache_hbm, value_hbm, proj_hbm, residual_hbm, router_hbm,
    gate_hbm, up_hbm, down_hbm, hidden_ref, out_ref,
    queries, cache, values, proj, residual_own, residual, router, gate, up, down,
    limits, context, heads_own, heads_all, mine, theirs, held, ids_all, local_v, picked, mixing, active,
    rows_v, sums, sums2, outbox, inbox, outbox2, inbox2, totals,
    load_sem, weight_sem, swap_sem, id_send, id_recv, res_send, res_recv,
    value_send, value_recv, heads_send, heads_recv, pair_send, pair_recv,
    piece_send, piece_recv, side_send, side_recv,
    both_send, both_recv, cross_send, cross_recv, back_send, back_recv,
):
    me = lax.axis_index("ep")
    core = lax.axis_index("tp")
    f32, bf16 = jnp.float32, jnp.bfloat16
    heads, _, latent, vdim = values.shape[0], values.shape[1], values.shape[1] * values.shape[2], values.shape[3]
    tokens = heads_own.shape[0]
    model = residual_own.shape[1]
    width = proj.shape[1]
    part = width // 2
    requests, columns, positions = cache.shape[1:]
    local = EXPERTS // count
    blocks = gate.shape[0] // local
    some = heads // 2
    half = tokens // 2
    place = ring_position(me, count)
    far = count // 2

    load_value = copy_here(value_hbm, values.at[:, me], load_sem.at[0])
    load_cache = copy_here(cache_hbm, cache.at[core], load_sem.at[1])
    load_residual = copy_here(residual_hbm, residual_own, load_sem.at[2])
    load_queries = copy_here(queries_hbm, queries, load_sem.at[3])
    load_proj = copy_here(proj_hbm, proj, load_sem.at[4])
    load_router = copy_here(router_hbm, router, load_sem.at[5])
    for number, (source, target) in enumerate(((gate_hbm, gate), (up_hbm, up), (down_hbm, down))):
        for expert in range(local):
            span = pl.ds(expert * blocks, blocks)
            pltpu.make_async_copy(source.at[span], target.at[span], weight_sem.at[number, expert]).start()
    ids_all[me] = meta_ref[...]
    greet(count)

    load_value.wait()
    value_ring = Ring(
        count,
        lambda p: values.at[pl.ds(p * some, some), me],
        lambda block, p: values.at[pl.ds(p * some, some), block],
        value_send, value_recv,
    )
    value_ring.launch()
    load_cache.wait()
    swap = remote(cache.at[core], cache.at[core], swap_sem.at[0], swap_sem.at[1], {"tp": 1 - core})
    swap.start()
    load_residual.wait()
    spreads = []
    for step in range(1, count):
        peer = lax.rem(me + step, count)
        column = pl.multiple_of(peer * width + core * part, part)
        spreads.append(
            remote(
                residual_own.at[:, pl.ds(column, part)], residual.at[me],
                res_send.at[step - 1], res_recv.at[step - 1], {"ep": peer},
            )
        )
        spreads.append(
            remote(
                ids_all.at[me], ids_all.at[me], id_send.at[step - 1], id_recv.at[step - 1], {"ep": peer}
            )
        )
    for copy in spreads:
        copy.start()
    residual[me] = residual_own[:, pl.ds(pl.multiple_of(me * width + core * part, part), part)]

    meta = meta_ref[...]
    visible = meta[TOPK : TOPK + 1, :tokens]
    request = meta[TOPK + 1 : TOPK + 2, :tokens]
    row_token = lax.broadcasted_iota(jnp.int32, (tokens * heads, tokens), 0) // heads
    own_token = row_token == lax.broadcasted_iota(jnp.int32, (tokens * heads, tokens), 1)
    for r in range(requests):
        seen = jnp.where(request == r, visible, 0).astype(f32)
        limits[:, r : r + 1] = jnp.sum(jnp.where(own_token, seen, 0.0), axis=1, keepdims=True)

    def attend(start):
        rows = pl.ds(start, ROWS)
        asked = queries[rows, :]
        lane = lax.broadcasted_iota(jnp.int32, (ROWS, positions), 1).astype(f32)
        scored = []
        peak = None
        for r in range(requests):
            limit = limits[rows, r : r + 1]
            for side in range(2):
                score = jnp.dot(asked, cache[side, r], preferred_element_type=f32) * score_scale
                score = jnp.where(lane + float(side * positions) < limit, score, -jnp.inf)
                scored.append(score)
                top = jnp.max(score, axis=1, keepdims=True)
                peak = top if peak is None else jnp.maximum(peak, top)
        total, summed = None, None
        for number, score in enumerate(scored):
            weight = jnp.exp(score - peak).astype(bf16)
            amount = jnp.sum(weight.astype(f32), axis=1, keepdims=True)
            r, side = number // 2, number % 2
            term = lax.dot_general(
                weight, cache[side, r, :latent, :], (((1,), (1,)), ((), ())), preferred_element_type=f32
            )
            total = amount if total is None else total + amount
            summed = term if summed is None else summed + term
        summed = summed / total
        for piece in range(latent // 128):
            context[piece, rows, :] = summed[:, piece * 128 : (piece + 1) * 128]

    load_queries.wait()
    value_ring.relay(1)
    swap.wait_recv()
    chunks = list(range(0, tokens * heads, ROWS))
    done = 0
    for step in range(2, far + 1):
        until = -(-len(chunks) * (step - 1) // (far - 1)) if step < far else len(chunks)
        for start in chunks[done:until]:
            attend(start)
        done = until
        value_ring.relay(step)
    for h in range(heads):
        rows = jnp.concatenate(
            [context[piece, pl.ds(h, tokens, stride=heads), :] for piece in range(latent // 128)], axis=1
        ).astype(bf16)
        heads_own[:, h * vdim : (h + 1) * vdim] = jnp.dot(
            rows, values[h].reshape(latent, vdim), preferred_element_type=f32
        ).astype(bf16)

    heads_ring = Ring(
        count,
        lambda p: heads_own.at[pl.ds(p * half, half)],
        lambda block, p: heads_all.at[block, pl.ds(p * half, half)],
        heads_send, heads_recv,
    )
    heads_ring.launch()
    load_proj.wait()
    for copy in spreads:
        copy.wait_recv()
    load_router.wait()
    pieces = Pieces(count, held, piece_send, piece_recv, side_send, side_recv)
    pairs = {}

    def block_at(offset):
        return ring_index(place + offset, count)

    def project(number):
        rows = heads_own[...] if number == 0 else heads_all[block_at(offset_of(number, count))]
        product = jnp.dot(rows, proj[...], preferred_element_type=f32)
        mine[number, 0] = product[:, :part]
        mine[number, 1] = product[:, part:]
        copy = remote(
            mine.at[number, 1 - core], theirs.at[number], pair_send.at[number], pair_recv.at[number],
            {"tp": 1 - core},
        )
        copy.start()
        pairs[number] = copy

    def conclude(number):
        pairs[number].wait_recv()
        block = block_at(offset_of(number, count))
        attention = mine[number, core] + theirs[number]
        held[block, me, core] = (residual[block].astype(f32) + attention).astype(bf16)
        pieces.launch(number)

    expert_row = lax.broadcasted_iota(jnp.int32, (EXPERTS, tokens), 0)
    before = (
        lax.broadcasted_iota(jnp.int32, (tokens, tokens), 0)
        < lax.broadcasted_iota(jnp.int32, (tokens, tokens), 1)
    ).astype(bf16)
    slot = lax.broadcasted_iota(jnp.int32, (local, CAP, tokens), 1).astype(f32)

    def route(offset):
        pieces.settle(offset)
        block = block_at(offset)
        index = offset % count
        wide = jnp.concatenate(
            [held[block, e, c] for e in range(count) for c in range(2)], axis=1
        ).astype(f32)
        scale = lax.rsqrt(jnp.mean(wide * wide, axis=1, keepdims=True) + epsilon)
        normed = (wide * scale * gain_ref[...]).astype(bf16)
        logits = lax.dot_general(
            router[...], normed, (((1,), (1,)), ((), ())), preferred_element_type=f32
        )
        ids = ids_all[block][:TOPK, :tokens]
        named = expert_row == ids[0:1]
        for k in range(1, TOPK):
            named = named | (expert_row == ids[k : k + 1])
        logits = jnp.where(named, logits, -jnp.inf)
        raised = jnp.exp(logits - jnp.max(logits, axis=0, keepdims=True))
        share = raised / jnp.sum(raised, axis=0, keepdims=True)
        local_v[0] = named.astype(f32)
        local_v[1] = share
        first = pl.ds(pl.multiple_of(me * local, local), local)
        here = local_v[0, first, :]
        share_here = local_v[1, first, :].astype(bf16).astype(f32)
        rank = jnp.dot(here.astype(bf16), before, preferred_element_type=f32)
        hits = (here[:, None, :] > 0.5) & (rank[:, None, :] == slot)
        mixing[index] = (
            jnp.where(hits, share_here[:, None, :], 0.0).reshape(local * CAP, tokens).astype(bf16)
        )
        chosen = jnp.dot(
            jnp.where(hits, 1.0, 0.0).reshape(local * CAP, tokens).astype(bf16), normed,
            preferred_element_type=f32,
        )
        for e in range(local):
            picked[e, pl.ds(index * CAP, CAP), :] = chosen[e * CAP : (e + 1) * CAP]

    for turn in range(2 * far + 1):
        if 1 <= turn <= far:
            heads_ring.relay(turn)
        if turn <= far:
            for number in group_of(turn, count):
                project(number)
        for group in range(far + 1):
            if 1 <= turn - group <= far:
                for number in group_of(group, count):
                    pieces.relay(turn - group, number)
        if turn <= far:
            for number in group_of(turn, count):
                conclude(number)
        if turn >= far:
            for offset in sorted({2 * far - turn, turn - 2 * far}):
                if offset != -far:
                    route(offset)

    hidden_ref[...] = jnp.concatenate(
        [held[me, (count // 2) * core + e, c] for e in range(count // 2) for c in range(2)], axis=1
    )

    def weights(number, expert):
        span = pl.ds(expert * blocks, blocks)
        source, target = ((gate_hbm, gate), (up_hbm, up), (down_hbm, down))[number]
        return pltpu.make_async_copy(source.at[span], target.at[span], weight_sem.at[number, expert])

    inner = blocks * gate.shape[1]

    def excite(expert, carry):
        weights(0, expert).wait()
        weights(1, expert).wait()
        span = pl.ds(expert * blocks, blocks)
        slots = picked[expert].astype(bf16)
        dims = (((1,), (1,)), ((), ()))
        gate_t = lax.dot_general(gate[span].reshape(inner, model), slots, dims, preferred_element_type=f32)
        up_t = lax.dot_general(up[span].reshape(inner, model), slots, dims, preferred_element_type=f32)
        active_t = gate_t / (1.0 + jnp.exp(-gate_t)) * up_t
        active[expert] = active_t.T.astype(bf16)
        return carry

    lax.fori_loop(0, local, excite, 0)
    for expert in range(local):
        weights(2, expert).wait()

    piece = sums.shape[4]
    turns = sums.shape[0]
    side_width = model // 2
    twin = me + 1 - 2 * lax.rem(me, 2)
    pair = count // 2
    steps = list(range(1, pair)) + [0]
    near_order = [lax.rem(me + 2 * step, count) for step in steps]
    twin_order = [lax.rem(twin + 2 * step, count) for step in steps]
    boths, crosses, backs = {}, {}, {}

    def lower(turn):
        def one(expert, carry):
            span = pl.ds(expert * blocks, blocks)
            for c in range(2):
                column = pl.ds(c * side_width + turn * piece, piece)
                rows_v[expert, :, c * piece : (c + 1) * piece] = jnp.dot(
                    active[expert], down[span, :, column].reshape(inner, piece),
                    preferred_element_type=f32,
                )
            return carry

        lax.fori_loop(0, local, one, 0)
        for offset in range(count):
            rows = jnp.concatenate(
                [rows_v[e, offset * CAP : (offset + 1) * CAP, :] for e in range(local)], axis=0
            ).astype(bf16)
            mixed = lax.dot_general(
                mixing[offset], rows, (((0,), (0,)), ((), ())), preferred_element_type=f32
            ).astype(bf16)
            block = block_at(offset)
            for c in range(2):
                sums[turn, c, block] = mixed[:, c * piece : (c + 1) * piece]
        boths[turn] = remote(
            sums.at[turn, 1 - core], sums2.at[turn], both_send.at[turn], both_recv.at[turn],
            {"tp": 1 - core},
        )
        boths[turn].start()

    def added(turn, block):
        return sums[turn, core, block].astype(f32) + sums2[turn, block].astype(f32)

    def cross(turn):
        boths[turn].wait_recv()
        for i, block in enumerate(twin_order):
            outbox[turn, i] = added(turn, block).astype(bf16)
        crosses[turn] = remote(
            outbox.at[turn], inbox.at[turn], cross_send.at[turn], cross_recv.at[turn], {"ep": twin}
        )
        crosses[turn].start()

    def back(turn):
        crosses[turn].wait_recv()
        for i, block in enumerate(near_order):
            total = added(turn, block) + inbox[turn, i].astype(f32)
            if i == pair - 1:
                totals[turn] = total
                continue
            outbox2[turn, i] = total.astype(bf16)
            backs[turn, i] = remote(
                outbox2.at[turn, i], inbox2.at[turn, i], back_send.at[turn, i], back_recv.at[turn, i],
                {"ep": block},
            )
            backs[turn, i].start()

    def end(turn):
        total = totals[turn]
        for i in range(pair - 1):
            backs[turn, i].wait_recv()
            total = total + inbox2[turn, i].astype(f32)
        out_ref[:, turn * piece : (turn + 1) * piece] = total.astype(bf16)

    for turn in range(turns):
        lower(turn)
        if turn >= 1:
            cross(turn - 1)
    cross(turns - 1)
    for turn in range(turns):
        back(turn)
    for turn in range(turns):
        end(turn)

    value_ring.finish()
    heads_ring.finish()
    pieces.finish()
    swap.wait_send()
    for copy in spreads:
        copy.wait_send()
    for group in (pairs, boths, crosses, backs):
        for copy in group.values():
            copy.wait_send()


def dma(*shape):
    return pltpu.SemaphoreType.DMA(shape)


TURNS = 4


def lean_body(
    queries,
    latent_cache,
    residual,
    token_request,
    token_visible,
    value_proj,
    out_proj,
    norm_gain,
    router,
    expert_ids,
    gate_weight,
    up_weight,
    down_weight,
):
    count = lax.axis_size("ep")
    tokens, heads, columns = queries.shape
    requests, positions, _ = latent_cache.shape
    model = residual.shape[1]
    bf16, f32 = jnp.bfloat16, jnp.float32
    shape = jax.ShapeDtypeStruct
    far = count // 2
    local = EXPERTS // count
    width = out_proj.shape[1]
    slots = count * CAP
    blocks = gate_weight.shape[0] // local
    hidden_here = gate_weight.shape[2]
    piece = model // 2 // TURNS
    meta = jnp.concatenate([expert_ids.T, token_visible[None], token_request[None]], axis=0)
    meta = jnp.pad(meta, ((0, 8 - meta.shape[0]), (0, 128 - tokens)))
    whole = pl.BlockSpec(memory_space=pltpu.VMEM)
    anywhere = pl.BlockSpec(memory_space=pl.ANY)
    vmem = pltpu.VMEM
    weight = (gate_weight.shape[0], hidden_here, model)
    hidden, expert_out = pl.pallas_call(
        functools.partial(layer_kernel, count),
        out_shape=(shape((tokens, model // 2), bf16), shape((tokens, model // 2), bf16)),
        in_specs=[whole] * 2 + [anywhere] * 9,
        out_specs=(whole, whole),
        scratch_shapes=[
            vmem((tokens * heads, columns), bf16),
            vmem((2, requests, columns, positions), bf16),
            vmem((heads, count) + value_proj.shape[1:], bf16),
            vmem(out_proj.shape, bf16),
            vmem((tokens, model), bf16),
            vmem((count, tokens, width // 2), bf16),
            vmem((EXPERTS, model), bf16),
            vmem(weight, bf16),
            vmem(weight, bf16),
            vmem(weight, bf16),
            vmem((tokens * heads, 128), f32),
            vmem((LATENT // 128, tokens * heads, 128), f32),
            vmem((tokens, heads * VDIM), bf16),
            vmem((count, tokens, heads * VDIM), bf16),
            vmem((count, 2, tokens, width // 2), f32),
            vmem((count, tokens, width // 2), f32),
            vmem((count, count, 2, tokens, width // 2), bf16),
            vmem((count, 8, 128), jnp.int32),
            vmem((2, EXPERTS, tokens), f32),
            vmem((local, slots, model), f32),
            vmem((count, local * CAP, tokens), bf16),
            vmem((local, slots, blocks * hidden_here), bf16),
            vmem((local, slots, 2 * piece), f32),
            vmem((TURNS, 2, count, tokens, piece), bf16),
            vmem((TURNS, count, tokens, piece), bf16),
            vmem((TURNS, far, tokens, piece), bf16),
            vmem((TURNS, far, tokens, piece), bf16),
            vmem((TURNS, far - 1, tokens, piece), bf16),
            vmem((TURNS, far - 1, tokens, piece), bf16),
            vmem((TURNS, tokens, piece), f32),
            dma(6), dma(3, local), dma(2), dma(count - 1), dma(count - 1), dma(count - 1), dma(count - 1),
            dma(2, far, 2), dma(2, far, 2), dma(2, far, 2), dma(2, far, 2), dma(count), dma(count),
            dma(count, 2, far), dma(count, 2, far), dma(count, count), dma(count, count),
            dma(TURNS), dma(TURNS), dma(TURNS), dma(TURNS), dma(TURNS, far - 1), dma(TURNS, far - 1),
        ],
        compiler_params=pltpu.CompilerParams(
            collective_id=0, has_side_effects=True, vmem_limit_bytes=63 * 2**20
        ),
    )(
        meta, norm_gain.reshape(1, model), queries.reshape(tokens * heads, columns),
        jnp.swapaxes(latent_cache, 1, 2), value_proj, out_proj, residual, router.T,
        jnp.swapaxes(gate_weight, 1, 2), jnp.swapaxes(up_weight, 1, 2), down_weight,
    )
    return (hidden, expert_out)


LEAN_BYTES = 8 * 2**20


def choose(mesh):
    count = mesh.shape["ep"]

    def layer(*args):
        tokens, model = args[2].shape
        fits = count * tokens * model * 2 <= LEAN_BYTES
        even = count % 2 == 0 and count >= 4 and tokens % 32 == 0 and EXPERTS % count == 0
        if fits and even and mesh.shape["tp"] == 2:
            return lean_body(*args)
        return body(*args)

    return layer


def solution(mesh):
    return jax.shard_map(
        choose(mesh),
        mesh=mesh,
        in_specs=(
            P(("grp", "ep"), "tp", None),
            P(("grp", "ep"), "tp", None),
            P(("grp", "ep"), None),
            P(("grp", "ep")),
            P(("grp", "ep")),
            P("tp", "ep", None),
            P("tp", "ep"),
            P(),
            P(),
            P(("grp", "ep"), None),
            P("ep", None, "tp"),
            P("ep", None, "tp"),
            P("ep", "tp", None),
        ),
        out_specs=(P(("grp", "ep"), "tp"), P(("grp", "ep"), "tp")),
        check_vma=False,
    )
```

```python
import functools

import jax
import jax.numpy as jnp
from jax import lax
from jax.experimental import pallas as pl
from jax.experimental.pallas import tpu as pltpu
from jax.sharding import PartitionSpec as P

LATENT = 512
VDIM = 128
EXPERTS = 64
TOPK = 6
GROUPS = 2
CAP = 8
PIECES = 128
MESH = pl.DeviceIdType.MESH


score_scale = 192.0 ** (-0.5)
epsilon = 1e-06


def masked_scores(queries, block_rows, token_request, token_visible):
    per_request = block_rows.shape[1]
    flat_rows = block_rows.reshape(-1, block_rows.shape[2])
    scores = (
        jnp.einsum("thc,kc->thk", queries, flat_rows, preferred_element_type=jnp.float32)
        * score_scale
    )
    column = jnp.arange(flat_rows.shape[0], dtype=jnp.int32)
    owner_id = column // per_request
    position = column % per_request
    allowed = (owner_id[None, :] == token_request[:, None]) & (
        position[None, :] < token_visible[:, None]
    )
    return (jnp.where(allowed[:, None, :], scores, -jnp.inf), flat_rows)


def weighted_rows(scores, row_peak, flat_rows):
    weights = jnp.exp(scores - row_peak[:, :, None]).astype(jnp.bfloat16)
    totals = jnp.sum(weights.astype(jnp.float32), axis=2)
    summed = jnp.einsum(
        "thk,kc->thc", weights, flat_rows[:, :LATENT], preferred_element_type=jnp.float32
    )
    return (summed, totals)


def expert_block(arrived, gate_weight, up_weight, down_weight):
    gate_vals = jnp.einsum("prd,pdf->prf", arrived, gate_weight, preferred_element_type=jnp.float32)
    up_vals = jnp.einsum("prd,pdf->prf", arrived, up_weight, preferred_element_type=jnp.float32)
    activated = (jax.nn.silu(gate_vals) * up_vals).astype(jnp.bfloat16)
    return jnp.einsum(
        "prf,pfd->prd", activated, down_weight, preferred_element_type=jnp.float32
    ).astype(jnp.bfloat16)


def body(
    queries,
    latent_cache,
    residual,
    token_request,
    token_visible,
    value_proj,
    out_proj,
    norm_gain,
    router,
    expert_ids,
    gate_weight,
    up_weight,
    down_weight,
):
    all_rows = lax.all_gather(latent_cache, "tp", axis=1, tiled=True)
    scores, flat_rows = masked_scores(queries, all_rows, token_request, token_visible)
    summed, totals = weighted_rows(scores, jnp.max(scores, axis=2), flat_rows)
    context = (summed / totals[:, :, None]).astype(jnp.bfloat16)
    tokens_here = context.shape[0]
    heads_here = context.shape[1]
    head_values = jnp.einsum(
        "thl,hlv->thv",
        context,
        lax.all_gather(value_proj, "ep", axis=1, tiled=True),
        preferred_element_type=jnp.float32,
    )
    heads_out = head_values.astype(jnp.bfloat16).reshape(tokens_here, heads_here * VDIM)
    column_block = jnp.dot(
        lax.all_gather(heads_out, "ep", axis=0, tiled=True),
        out_proj,
        preferred_element_type=jnp.float32,
    )
    attention_part = lax.all_to_all(column_block, "ep", split_axis=0, concat_axis=1, tiled=True)
    attention = lax.psum(attention_part, "tp")
    hidden = (residual.astype(jnp.float32) + attention).astype(jnp.bfloat16)
    hidden_wide = hidden.astype(jnp.float32)
    normed = (
        hidden_wide
        * lax.rsqrt(jnp.mean(hidden_wide * hidden_wide, axis=1, keepdims=True) + epsilon)
        * norm_gain
    ).astype(jnp.bfloat16)
    logits = jnp.dot(normed, router, preferred_element_type=jnp.float32)
    gate_share = jax.nn.softmax(jnp.take_along_axis(logits, expert_ids, axis=1), axis=1).astype(
        jnp.bfloat16
    )
    flat_ids = expert_ids.reshape(-1)
    position_id = jnp.arange(flat_ids.shape[0], dtype=jnp.int32)
    earlier = (flat_ids[:, None] == flat_ids[None, :]) & (
        position_id[None, :] < position_id[:, None]
    )
    slot_ids = (flat_ids * CAP + jnp.sum(earlier.astype(jnp.int32), axis=1)).reshape(
        tokens_here, TOPK
    )
    targets = jnp.arange(EXPERTS * CAP, dtype=jnp.int32)
    matches = slot_ids[:, :, None] == targets[None, None, :]
    picker = jnp.any(matches, axis=1).T.astype(jnp.bfloat16)
    model_width = normed.shape[1]
    mixing = jnp.sum(
        jnp.where(matches, gate_share[:, :, None], jnp.zeros((), jnp.bfloat16)), axis=1
    )
    mixing = jnp.broadcast_to(
        mixing.reshape(tokens_here, EXPERTS, 1, CAP), (tokens_here, EXPERTS, GROUPS, CAP)
    ).reshape(tokens_here, PIECES * CAP)
    core_count = lax.axis_size("tp")
    half_width = model_width // core_count
    core_start = lax.axis_index("tp") * half_width
    outgoing = jnp.dot(picker, normed, preferred_element_type=jnp.float32).astype(jnp.bfloat16)
    outgoing = jnp.broadcast_to(
        outgoing.reshape(EXPERTS, 1, CAP, model_width), (EXPERTS, GROUPS, CAP, model_width)
    ).reshape(PIECES, CAP, model_width)
    arrived = lax.all_to_all(outgoing, "ep", split_axis=0, concat_axis=1, tiled=True)
    partial_out = expert_block(arrived, gate_weight, up_weight, down_weight)
    returned = lax.all_to_all(partial_out, "ep", split_axis=1, concat_axis=0, tiled=True)
    routed = jnp.dot(
        mixing, returned.reshape(PIECES * CAP, model_width), preferred_element_type=jnp.float32
    )
    expert_out = lax.psum_scatter(
        routed.astype(jnp.bfloat16), "tp", scatter_dimension=1, tiled=True
    )
    hidden_part = lax.dynamic_slice_in_dim(hidden, core_start, half_width, 1)
    return (hidden_part, expert_out)


def ring_position(index, count):
    half = lax.div(index, 2)
    return half + lax.rem(index, 2) * (count - 1 - 2 * half)


def ring_index(place, count):
    place = lax.rem(place + count, count)
    upper = lax.div(place, count // 2)
    return 2 * place + upper * (2 * count - 1 - 4 * place)


def greet(count):
    me = lax.axis_index("ep")
    core = lax.axis_index("tp")
    barrier = pltpu.get_barrier_semaphore()
    for step in range(1, count):
        pl.semaphore_signal(
            barrier, inc=1, device_id={"ep": lax.rem(me + step, count)}, device_id_type=MESH
        )
    pl.semaphore_signal(barrier, inc=1, device_id={"tp": 1 - core}, device_id_type=MESH)
    pl.semaphore_wait(barrier, count)


def remote(src, dst, send_sem, recv_sem, where):
    return pltpu.make_async_remote_copy(
        src_ref=src,
        dst_ref=dst,
        send_sem=send_sem,
        recv_sem=recv_sem,
        device_id=where,
        device_id_type=MESH,
    )


def drain(ref, sem):
    pltpu.make_async_copy(ref, ref, sem).wait()


def copy_here(src, dst, sem):
    copy = pltpu.make_async_copy(src, dst, sem)
    copy.start()
    return copy


class Ring:
    def __init__(self, count, own, slot, send_sem, recv_sem):
        self.count = count
        self.place = ring_position(lax.axis_index("ep"), count)
        self.far = count // 2
        self.near = count - 1 - self.far
        self.to = (ring_index(self.place + 1, count), ring_index(self.place - 1, count))
        self.own, self.slot = own, slot
        self.send_sem, self.recv_sem = send_sem, recv_sem
        self.hops = {}
        self.order = [
            (way, part)
            for turn in range(2)
            for pair in range(PARTS // 2)
            for way in range(2)
            for part in (2 * pair + (way + turn) % 2,)
        ]

    def reach(self, way, part):
        return self.far if way == part % 2 else self.near

    def origin(self, way, step):
        return ring_index(self.place - step if way == 0 else self.place + step, self.count)

    def hop(self, way, step, part):
        if step > self.reach(way, part):
            return
        block = self.origin(way, step - 1)
        self.hops[way, step, part] = remote(
            self.own(part) if step == 1 else self.slot(block, part),
            self.slot(block, part),
            self.send_sem,
            self.recv_sem.at[way, step - 1, part],
            {"ep": self.to[way]},
        )
        self.hops[way, step, part].start()

    def launch(self):
        for way, part in self.order:
            self.hop(way, 1, part)

    def relay(self, step):
        for way, part in self.order:
            if step <= self.reach(way, part):
                self.hops[way, step, part].wait_recv()
                self.hop(way, step + 1, part)

def number_of(offset, count):
    far = count // 2
    offset = offset % count
    if offset > far:
        offset -= count
    if offset == 0:
        return 0
    if offset == far:
        return count - 1
    return -2 * offset - 1 if offset < 0 else 2 * offset


def offset_of(number, count):
    if number == count - 1:
        return count // 2
    step = (number + 1) // 2
    return -step if number % 2 else step


class Pieces:
    def __init__(self, count, held, ring_send, ring_recv, side_send, side_recv):
        self.count = count
        self.place = ring_position(lax.axis_index("ep"), count)
        self.core = lax.axis_index("tp")
        self.far = count // 2
        self.near = count - 1 - self.far
        self.to = (ring_index(self.place + 1, count), ring_index(self.place - 1, count))
        self.held = held
        self.sems = (ring_send, ring_recv, side_send, side_recv)
        self.hops, self.sides = {}, {}

    def piece(self, offset, number):
        block = ring_index(self.place + offset + offset_of(number, self.count), self.count)
        return self.held.at[block, ring_index(self.place + offset, self.count), self.core]

    def reach(self, way, number):
        return self.far if number % 2 == way else self.near

    def hop(self, way, step, number):
        if step > self.reach(way, number):
            return
        ref = self.piece(-(step - 1) if way == 0 else step - 1, number)
        copy = remote(
            ref, ref, self.sems[0], self.sems[1].at[number, way, step - 1], {"ep": self.to[way]}
        )
        copy.start()
        self.hops[way, step, number] = copy

    def side(self, offset, number):
        ref = self.piece(offset, number)
        where = (offset + offset_of(number, self.count)) % self.count
        remote(ref, ref, self.sems[2], self.sems[3].at[where], {"tp": 1 - self.core}).start()

    def launch(self, number):
        for turn in range(2):
            self.hop((number + turn) % 2, 1, number)
        self.side(0, number)

    def relay(self, step, number):
        for turn in range(2):
            way = (number + turn) % 2
            if step <= self.reach(way, number):
                self.hops[way, step, number].wait_recv()
                self.hop(way, step + 1, number)
                self.side(-step if way == 0 else step, number)

    def settle(self, offset):
        drain(self.held.at[0, :, 0], self.sems[3].at[offset % self.count])

    def finish(self):
        drain(self.held.at[: self.count - 1, :, 0], self.sems[0])
        drain(self.held.at[:, :, 0], self.sems[2])


def group_of(step, count):
    far = count // 2
    if step == 0:
        return [0]
    if step == far:
        return [count - 1]
    return [2 * step - 1, 2 * step]


ROWS = 256
PARTS = 4


def layer_kernel(
    count, ids_ref, visible_ref, request_ref, gain_ref, queries_hbm, cache_hbm, value_hbm, proj_hbm, residual_hbm, router_hbm,
    gate_hbm, up_hbm, down_hbm, hidden_ref, out_ref,
    queries, cache, values, proj, residual_own, residual, router, gate, up, down,
    limits, context, heads_own, heads_all, mine, theirs, held, ids_all, local_v, picked, mixing, active,
    sums, sums2, outbox, inbox, outbox2, inbox2, totals,
    load_sem, excite_sem, lower_sem, swap_sem, id_sem, res_sem,
    value_send, value_recv, heads_send, heads_recv, pair_send, pair_recv,
    piece_send, piece_recv, side_send, side_recv,
    both_send, both_recv, cross_send, cross_recv, back_send, back_recv,
):
    me = lax.axis_index("ep")
    core = lax.axis_index("tp")
    f32, bf16 = jnp.float32, jnp.bfloat16
    heads, _, latent, vdim = values.shape[0], values.shape[1], values.shape[1] * values.shape[2], values.shape[3]
    tokens = heads_own.shape[0]
    model = residual_own.shape[1]
    width = proj.shape[1]
    part = width // 2
    requests, columns, positions = cache.shape[1:]
    local = EXPERTS // count
    blocks = gate.shape[0] // local
    some = heads // PARTS
    half = tokens // PARTS
    place = ring_position(me, count)
    far = count // 2

    load_value = copy_here(value_hbm, values.at[:, me], load_sem.at[0])
    load_cache = copy_here(cache_hbm, cache.at[core], load_sem.at[1])
    load_residual = copy_here(residual_hbm, residual_own, load_sem.at[2])
    load_queries = copy_here(queries_hbm, queries, load_sem.at[3])
    load_proj = copy_here(proj_hbm, proj, load_sem.at[4])
    load_router = copy_here(router_hbm, router, load_sem.at[5])
    ids_all[me, :TOPK, :tokens] = ids_ref[...]
    greet(count)

    load_value.wait()
    value_ring = Ring(
        count,
        lambda p: values.at[pl.ds(p * some, some), me],
        lambda block, p: values.at[pl.ds(p * some, some), block],
        value_send, value_recv,
    )
    value_ring.launch()
    load_cache.wait()
    swap = remote(cache.at[core], cache.at[core], swap_sem.at[0], swap_sem.at[1], {"tp": 1 - core})
    swap.start()
    load_residual.wait()
    load_queries.wait()
    load_proj.wait()
    load_router.wait()
    for expert in range(local):
        span = pl.ds(expert * blocks, blocks)
        for source, target in ((gate_hbm, gate), (up_hbm, up)):
            pltpu.make_async_copy(source.at[span], target.at[span], excite_sem.at[expert]).start()
    load_down = copy_here(down_hbm, down, lower_sem)
    spreads = []
    for step in range(1, count):
        peer = lax.rem(me + step, count)
        column = pl.multiple_of(peer * width + core * part, part)
        spreads.append(
            remote(residual_own.at[:, pl.ds(column, part)], residual.at[me], res_sem.at[0], res_sem.at[1], {"ep": peer})
        )
        spreads.append(remote(ids_all.at[me], ids_all.at[me], id_sem.at[0], id_sem.at[1], {"ep": peer}))
    residual[me] = residual_own[:, pl.ds(pl.multiple_of(me * width + core * part, part), part)]

    visible, request = visible_ref[...], request_ref[...]
    row_token = lax.broadcasted_iota(jnp.int32, (tokens * heads, tokens), 0) // heads
    own_token = row_token == lax.broadcasted_iota(jnp.int32, (tokens * heads, tokens), 1)
    for r in range(requests):
        seen = jnp.where(request == r, visible, 0).astype(f32)
        limits[:, r : r + 1] = jnp.sum(jnp.where(own_token, seen, 0.0), axis=1, keepdims=True)

    def attend(start):
        rows = pl.ds(start, ROWS)
        asked = queries[rows, :]
        lane = lax.broadcasted_iota(jnp.int32, (ROWS, positions), 1).astype(f32)
        scored = []
        peak = None
        for r in range(requests):
            limit = limits[rows, r : r + 1]
            for side in range(2):
                score = jnp.dot(asked, cache[side, r], preferred_element_type=f32) * score_scale
                score = jnp.where(lane + float(side * positions) < limit, score, -jnp.inf)
                scored.append(score)
                top = jnp.max(score, axis=1, keepdims=True)
                peak = top if peak is None else jnp.maximum(peak, top)
        total, summed = None, None
        for number, score in enumerate(scored):
            weight = jnp.exp(score - peak).astype(bf16)
            amount = jnp.sum(weight.astype(f32), axis=1, keepdims=True)
            r, side = number // 2, number % 2
            term = lax.dot_general(
                weight, cache[side, r, :latent, :], (((1,), (1,)), ((), ())), preferred_element_type=f32
            )
            total = amount if total is None else total + amount
            summed = term if summed is None else summed + term
        summed = summed / total
        for piece in range(latent // 128):
            context[piece, rows, :] = summed[:, piece * 128 : (piece + 1) * 128]

    value_ring.relay(1)
    swap.wait_recv()
    chunks = list(range(0, tokens * heads, ROWS))
    done = 0
    for step in range(2, far + 1):
        until = -(-len(chunks) * (step - 1) // (far - 1)) if step < far else len(chunks)
        for start in chunks[done:until]:
            attend(start)
        done = until
        value_ring.relay(step)
        if step == 2:
            for copy in spreads:
                copy.start()
    for h in range(heads):
        rows = jnp.concatenate(
            [context[piece, pl.ds(h, tokens, stride=heads), :] for piece in range(latent // 128)], axis=1
        ).astype(bf16)
        heads_own[:, h * vdim : (h + 1) * vdim] = jnp.dot(
            rows, values[h].reshape(latent, vdim), preferred_element_type=f32
        ).astype(bf16)

    heads_ring = Ring(
        count,
        lambda p: heads_own.at[pl.ds(p * half, half)],
        lambda block, p: heads_all.at[block, pl.ds(p * half, half)],
        heads_send, heads_recv,
    )
    heads_ring.launch()
    pieces = Pieces(count, held, piece_send, piece_recv, side_send, side_recv)
    pairs = {}

    def block_at(offset):
        return ring_index(place + offset, count)

    def project(number):
        rows = heads_own[...] if number == 0 else heads_all[block_at(offset_of(number, count))]
        product = jnp.dot(rows, proj[...], preferred_element_type=f32)
        mine[number, 0] = product[:, :part]
        mine[number, 1] = product[:, part:]
        copy = remote(
            mine.at[number, 1 - core], theirs.at[number], pair_send, pair_recv.at[number],
            {"tp": 1 - core},
        )
        copy.start()
        pairs[number] = copy

    def conclude(number):
        if number == 0:
            drain(residual.at[: count - 1], res_sem.at[1])
            drain(ids_all.at[: count - 1], id_sem.at[1])
        pairs[number].wait_recv()
        block = block_at(offset_of(number, count))
        attention = mine[number, core] + theirs[number]
        held[block, me, core] = (residual[block].astype(f32) + attention).astype(bf16)
        pieces.launch(number)

    expert_row = lax.broadcasted_iota(jnp.int32, (EXPERTS, tokens), 0)
    before = (
        lax.broadcasted_iota(jnp.int32, (tokens, tokens), 0)
        < lax.broadcasted_iota(jnp.int32, (tokens, tokens), 1)
    ).astype(bf16)
    slot = lax.broadcasted_iota(jnp.int32, (local, CAP, tokens), 1).astype(f32)

    def route(offset):
        pieces.settle(offset)
        block = block_at(offset)
        index = offset % count
        wide = jnp.concatenate(
            [held[block, e, c] for e in range(count) for c in range(2)], axis=1
        ).astype(f32)
        scale = lax.rsqrt(jnp.mean(wide * wide, axis=1, keepdims=True) + epsilon)
        normed = (wide * scale * gain_ref[...]).astype(bf16)
        logits = lax.dot_general(
            router[...], normed, (((1,), (1,)), ((), ())), preferred_element_type=f32
        )
        ids = ids_all[block][:TOPK, :tokens]
        named = expert_row == ids[0:1]
        for k in range(1, TOPK):
            named = named | (expert_row == ids[k : k + 1])
        logits = jnp.where(named, logits, -jnp.inf)
        raised = jnp.exp(logits - jnp.max(logits, axis=0, keepdims=True))
        share = raised / jnp.sum(raised, axis=0, keepdims=True)
        local_v[0] = named.astype(f32)
        local_v[1] = share
        first = pl.ds(pl.multiple_of(me * local, local), local)
        here = local_v[0, first, :]
        share_here = local_v[1, first, :].astype(bf16).astype(f32)
        rank = jnp.dot(here.astype(bf16), before, preferred_element_type=f32)
        hits = (here[:, None, :] > 0.5) & (rank[:, None, :] == slot)
        mixed = jnp.where(hits, share_here[:, None, :], 0.0).reshape(local * CAP, tokens)
        mixing[index] = mixed.T.astype(bf16)
        chosen = jnp.dot(
            jnp.where(hits, 1.0, 0.0).reshape(local * CAP, tokens).astype(bf16), normed,
            preferred_element_type=f32,
        )
        for e in range(local):
            picked[e, pl.ds(index * CAP, CAP), :] = chosen[e * CAP : (e + 1) * CAP]

    for turn in range(2 * far + 1):
        if 1 <= turn <= far:
            heads_ring.relay(turn)
        if turn <= far:
            for number in group_of(turn, count):
                project(number)
        for group in range(far + 1):
            if 1 <= turn - group <= far:
                for number in group_of(group, count):
                    pieces.relay(turn - group, number)
        if turn <= far:
            for number in group_of(turn, count):
                conclude(number)
        if turn >= far:
            for offset in sorted({2 * far - turn, turn - 2 * far}):
                if offset != -far:
                    route(offset)

    hidden_ref[...] = jnp.concatenate(
        [held[me, (count // 2) * core + e, c] for e in range(count // 2) for c in range(2)], axis=1
    )

    inner = blocks * gate.shape[1]

    def excite(expert, carry):
        drain(gate.at[: 2 * blocks], excite_sem.at[expert])
        span = pl.ds(expert * blocks, blocks)
        slots = picked[expert].astype(bf16)
        dims = (((1,), (1,)), ((), ()))
        gate_t = lax.dot_general(gate[span].reshape(inner, model), slots, dims, preferred_element_type=f32)
        up_t = lax.dot_general(up[span].reshape(inner, model), slots, dims, preferred_element_type=f32)
        active_t = gate_t / (1.0 + jnp.exp(-gate_t)) * up_t
        active[expert] = active_t.T.astype(bf16)
        return carry

    lax.fori_loop(0, local, excite, 0)
    load_down.wait()

    piece = sums.shape[4]
    turns = sums.shape[0]
    side_width = model // 2
    twin = me + 1 - 2 * lax.rem(me, 2)
    pair = count // 2
    steps = list(range(1, pair)) + [0]
    near_order = [lax.rem(me + 2 * step, count) for step in steps]
    twin_order = [lax.rem(twin + 2 * step, count) for step in steps]
    boths, crosses = {}, {}

    def lower(turn):
        rows = []
        for expert in range(local):
            span = pl.ds(expert * blocks, blocks)
            sides = [
                jnp.dot(
                    active[expert],
                    down[span, :, pl.ds(c * side_width + turn * piece, piece)].reshape(inner, piece),
                    preferred_element_type=f32,
                )
                for c in range(2)
            ]
            rows.append(jnp.concatenate(sides, axis=1))
        for offset in range(count):
            mine_rows = [row[offset * CAP : (offset + 1) * CAP] for row in rows]
            mixed = jnp.dot(
                mixing[offset], jnp.concatenate(mine_rows, axis=0).astype(bf16), preferred_element_type=f32
            ).astype(bf16)
            block = block_at(offset)
            for c in range(2):
                sums[turn, c, block] = mixed[:, c * piece : (c + 1) * piece]
        boths[turn] = remote(
            sums.at[turn, 1 - core], sums2.at[turn], both_send, both_recv.at[turn],
            {"tp": 1 - core},
        )
        boths[turn].start()

    def added(turn, block):
        return sums[turn, core, block].astype(f32) + sums2[turn, block].astype(f32)

    def cross(turn):
        boths[turn].wait_recv()
        for i, block in enumerate(twin_order):
            outbox[turn, i] = added(turn, block).astype(bf16)
        crosses[turn] = remote(
            outbox.at[turn], inbox.at[turn], cross_send, cross_recv.at[turn], {"ep": twin}
        )
        crosses[turn].start()

    def back(turn):
        crosses[turn].wait_recv()
        for i, block in enumerate(near_order):
            total = added(turn, block) + inbox[turn, i].astype(f32)
            if i == pair - 1:
                totals[turn] = total
                continue
            outbox2[turn, i] = total.astype(bf16)
            remote(
                outbox2.at[turn, i], inbox2.at[turn, i], back_send, back_recv.at[turn], {"ep": block}
            ).start()

    def end(turn):
        total = totals[turn]
        drain(inbox2.at[turn], back_recv.at[turn])
        for i in range(pair - 1):
            total = total + inbox2[turn, i].astype(f32)
        out_ref[:, turn * piece : (turn + 1) * piece] = total.astype(bf16)

    for turn in range(turns + 3):
        if turn < turns:
            lower(turn)
        if 1 <= turn <= turns:
            cross(turn - 1)
        if turn >= 3:
            back(turn - 3)
    for turn in range(turns):
        end(turn)

    drain(values.at[:, : count - 1], value_send)
    drain(heads_all.at[: count - 1], heads_send)
    pieces.finish()
    swap.wait_send()
    drain(residual.at[: count - 1], res_sem.at[0])
    drain(ids_all.at[: count - 1], id_sem.at[0])
    drain(theirs, pair_send)
    drain(sums2, both_send)
    drain(inbox, cross_send)
    drain(inbox2, back_send)


def dma(*shape):
    return pltpu.SemaphoreType.DMA(shape)


TURNS = 8


def lean_body(
    queries,
    latent_cache,
    residual,
    token_request,
    token_visible,
    value_proj,
    out_proj,
    norm_gain,
    router,
    expert_ids,
    gate_weight,
    up_weight,
    down_weight,
):
    count = lax.axis_size("ep")
    tokens, heads, columns = queries.shape
    requests, positions, _ = latent_cache.shape
    model = residual.shape[1]
    bf16, f32 = jnp.bfloat16, jnp.float32
    shape = jax.ShapeDtypeStruct
    far = count // 2
    local = EXPERTS // count
    width = out_proj.shape[1]
    slots = count * CAP
    blocks = gate_weight.shape[0] // local
    hidden_here = gate_weight.shape[2]
    piece = model // 2 // TURNS
    whole = pl.BlockSpec(memory_space=pltpu.VMEM)
    anywhere = pl.BlockSpec(memory_space=pl.ANY)
    vmem = pltpu.VMEM
    weight = (gate_weight.shape[0], hidden_here, model)
    hidden, expert_out = pl.pallas_call(
        functools.partial(layer_kernel, count),
        out_shape=(shape((tokens, model // 2), bf16), shape((tokens, model // 2), bf16)),
        in_specs=[whole] * 4 + [anywhere] * 9,
        out_specs=(whole, whole),
        scratch_shapes=[
            vmem((tokens * heads, columns), bf16),
            vmem((2, requests, columns, positions), bf16),
            vmem((heads, count) + value_proj.shape[1:], bf16),
            vmem(out_proj.shape, bf16),
            vmem((tokens, model), bf16),
            vmem((count, tokens, width // 2), bf16),
            vmem((EXPERTS, model), bf16),
            vmem(weight, bf16),
            vmem(weight, bf16),
            vmem(weight, bf16),
            vmem((tokens * heads, 128), f32),
            vmem((LATENT // 128, tokens * heads, 128), f32),
            vmem((tokens, heads * VDIM), bf16),
            vmem((count, tokens, heads * VDIM), bf16),
            vmem((count, 2, tokens, width // 2), f32),
            vmem((count, tokens, width // 2), f32),
            vmem((count, count, 2, tokens, width // 2), bf16),
            vmem((count, 8, 128), jnp.int32),
            vmem((2, EXPERTS, tokens), f32),
            vmem((local, slots, model), f32),
            vmem((count, tokens, local * CAP), bf16),
            vmem((local, slots, blocks * hidden_here), bf16),
            vmem((TURNS, 2, count, tokens, piece), bf16),
            vmem((TURNS, count, tokens, piece), bf16),
            vmem((TURNS, far, tokens, piece), bf16),
            vmem((TURNS, far, tokens, piece), bf16),
            vmem((TURNS, far - 1, tokens, piece), bf16),
            vmem((TURNS, far - 1, tokens, piece), bf16),
            vmem((TURNS, tokens, piece), f32),
            dma(6), dma(local), dma(), dma(2), dma(2), dma(2),
            dma(), dma(2, far, PARTS), dma(), dma(2, far, PARTS), dma(), dma(count),
            dma(), dma(count, 2, far), dma(), dma(count),
            dma(), dma(TURNS), dma(), dma(TURNS), dma(), dma(TURNS),
        ],
        compiler_params=pltpu.CompilerParams(
            collective_id=0, has_side_effects=True, vmem_limit_bytes=59 * 2**20
        ),
    )(
        expert_ids.T, token_visible[None], token_request[None], norm_gain[None], queries.reshape(tokens * heads, columns),
        jnp.swapaxes(latent_cache, 1, 2), value_proj, out_proj, residual, router.T,
        jnp.swapaxes(gate_weight, 1, 2), jnp.swapaxes(up_weight, 1, 2), down_weight,
    )
    return (hidden, expert_out)


LEAN_BYTES = 8 * 2**20


def choose(mesh):
    count = mesh.shape["ep"]

    def layer(*args):
        tokens, model = args[2].shape
        fits = count * tokens * model * 2 <= LEAN_BYTES
        even = count % 2 == 0 and count >= 4 and tokens % 32 == 0 and EXPERTS % count == 0
        if fits and even and mesh.shape["tp"] == 2:
            return lean_body(*args)
        return body(*args)

    return layer


def solution(mesh):
    return jax.shard_map(
        choose(mesh),
        mesh=mesh,
        in_specs=(
            P(("grp", "ep"), "tp", None),
            P(("grp", "ep"), "tp", None),
            P(("grp", "ep"), None),
            P(("grp", "ep")),
            P(("grp", "ep")),
            P("tp", "ep", None),
            P("tp", "ep"),
            P(),
            P(),
            P(("grp", "ep"), None),
            P("ep", None, "tp"),
            P("ep", None, "tp"),
            P("ep", "tp", None),
        ),
        out_specs=(P(("grp", "ep"), "tp"), P(("grp", "ep"), "tp")),
        check_vma=False,
    )
```

```python
import functools

import jax
import jax.numpy as jnp
from jax import lax
from jax.experimental import pallas as pl
from jax.experimental.pallas import tpu as pltpu
from jax.sharding import PartitionSpec as P

LATENT = 512
VDIM = 128
EXPERTS = 64
TOPK = 6
GROUPS = 2
CAP = 8
PIECES = 128
MESH = pl.DeviceIdType.MESH


score_scale = 192.0 ** (-0.5)
epsilon = 1e-06


def masked_scores(queries, block_rows, token_request, token_visible):
    per_request = block_rows.shape[1]
    flat_rows = block_rows.reshape(-1, block_rows.shape[2])
    scores = (
        jnp.einsum("thc,kc->thk", queries, flat_rows, preferred_element_type=jnp.float32)
        * score_scale
    )
    column = jnp.arange(flat_rows.shape[0], dtype=jnp.int32)
    owner_id = column // per_request
    position = column % per_request
    allowed = (owner_id[None, :] == token_request[:, None]) & (
        position[None, :] < token_visible[:, None]
    )
    return (jnp.where(allowed[:, None, :], scores, -jnp.inf), flat_rows)


def weighted_rows(scores, row_peak, flat_rows):
    weights = jnp.exp(scores - row_peak[:, :, None]).astype(jnp.bfloat16)
    totals = jnp.sum(weights.astype(jnp.float32), axis=2)
    summed = jnp.einsum(
        "thk,kc->thc", weights, flat_rows[:, :LATENT], preferred_element_type=jnp.float32
    )
    return (summed, totals)


def expert_block(arrived, gate_weight, up_weight, down_weight):
    gate_vals = jnp.einsum("prd,pdf->prf", arrived, gate_weight, preferred_element_type=jnp.float32)
    up_vals = jnp.einsum("prd,pdf->prf", arrived, up_weight, preferred_element_type=jnp.float32)
    activated = (jax.nn.silu(gate_vals) * up_vals).astype(jnp.bfloat16)
    return jnp.einsum(
        "prf,pfd->prd", activated, down_weight, preferred_element_type=jnp.float32
    ).astype(jnp.bfloat16)


def body(
    queries,
    latent_cache,
    residual,
    token_request,
    token_visible,
    value_proj,
    out_proj,
    norm_gain,
    router,
    expert_ids,
    gate_weight,
    up_weight,
    down_weight,
):
    all_rows = lax.all_gather(latent_cache, "tp", axis=1, tiled=True)
    scores, flat_rows = masked_scores(queries, all_rows, token_request, token_visible)
    summed, totals = weighted_rows(scores, jnp.max(scores, axis=2), flat_rows)
    context = (summed / totals[:, :, None]).astype(jnp.bfloat16)
    tokens_here = context.shape[0]
    heads_here = context.shape[1]
    head_values = jnp.einsum(
        "thl,hlv->thv",
        context,
        lax.all_gather(value_proj, "ep", axis=1, tiled=True),
        preferred_element_type=jnp.float32,
    )
    heads_out = head_values.astype(jnp.bfloat16).reshape(tokens_here, heads_here * VDIM)
    column_block = jnp.dot(
        lax.all_gather(heads_out, "ep", axis=0, tiled=True),
        out_proj,
        preferred_element_type=jnp.float32,
    )
    attention_part = lax.all_to_all(column_block, "ep", split_axis=0, concat_axis=1, tiled=True)
    attention = lax.psum(attention_part, "tp")
    hidden = (residual.astype(jnp.float32) + attention).astype(jnp.bfloat16)
    hidden_wide = hidden.astype(jnp.float32)
    normed = (
        hidden_wide
        * lax.rsqrt(jnp.mean(hidden_wide * hidden_wide, axis=1, keepdims=True) + epsilon)
        * norm_gain
    ).astype(jnp.bfloat16)
    logits = jnp.dot(normed, router, preferred_element_type=jnp.float32)
    gate_share = jax.nn.softmax(jnp.take_along_axis(logits, expert_ids, axis=1), axis=1).astype(
        jnp.bfloat16
    )
    flat_ids = expert_ids.reshape(-1)
    position_id = jnp.arange(flat_ids.shape[0], dtype=jnp.int32)
    earlier = (flat_ids[:, None] == flat_ids[None, :]) & (
        position_id[None, :] < position_id[:, None]
    )
    slot_ids = (flat_ids * CAP + jnp.sum(earlier.astype(jnp.int32), axis=1)).reshape(
        tokens_here, TOPK
    )
    targets = jnp.arange(EXPERTS * CAP, dtype=jnp.int32)
    matches = slot_ids[:, :, None] == targets[None, None, :]
    picker = jnp.any(matches, axis=1).T.astype(jnp.bfloat16)
    model_width = normed.shape[1]
    mixing = jnp.sum(
        jnp.where(matches, gate_share[:, :, None], jnp.zeros((), jnp.bfloat16)), axis=1
    )
    mixing = jnp.broadcast_to(
        mixing.reshape(tokens_here, EXPERTS, 1, CAP), (tokens_here, EXPERTS, GROUPS, CAP)
    ).reshape(tokens_here, PIECES * CAP)
    core_count = lax.axis_size("tp")
    half_width = model_width // core_count
    core_start = lax.axis_index("tp") * half_width
    outgoing = jnp.dot(picker, normed, preferred_element_type=jnp.float32).astype(jnp.bfloat16)
    outgoing = jnp.broadcast_to(
        outgoing.reshape(EXPERTS, 1, CAP, model_width), (EXPERTS, GROUPS, CAP, model_width)
    ).reshape(PIECES, CAP, model_width)
    arrived = lax.all_to_all(outgoing, "ep", split_axis=0, concat_axis=1, tiled=True)
    partial_out = expert_block(arrived, gate_weight, up_weight, down_weight)
    returned = lax.all_to_all(partial_out, "ep", split_axis=1, concat_axis=0, tiled=True)
    routed = jnp.dot(
        mixing, returned.reshape(PIECES * CAP, model_width), preferred_element_type=jnp.float32
    )
    expert_out = lax.psum_scatter(
        routed.astype(jnp.bfloat16), "tp", scatter_dimension=1, tiled=True
    )
    hidden_part = lax.dynamic_slice_in_dim(hidden, core_start, half_width, 1)
    return (hidden_part, expert_out)


def ring_position(index, count):
    half = lax.div(index, 2)
    return half + lax.rem(index, 2) * (count - 1 - 2 * half)


def ring_index(place, count):
    place = lax.rem(place + count, count)
    upper = lax.div(place, count // 2)
    return 2 * place + upper * (2 * count - 1 - 4 * place)


def greet(count):
    me = lax.axis_index("ep")
    core = lax.axis_index("tp")
    barrier = pltpu.get_barrier_semaphore()
    for step in range(1, count):
        pl.semaphore_signal(
            barrier, inc=1, device_id={"ep": lax.rem(me + step, count)}, device_id_type=MESH
        )
    pl.semaphore_signal(barrier, inc=1, device_id={"tp": 1 - core}, device_id_type=MESH)
    pl.semaphore_wait(barrier, count)


def remote(src, dst, send_sem, recv_sem, where):
    return pltpu.make_async_remote_copy(
        src_ref=src,
        dst_ref=dst,
        send_sem=send_sem,
        recv_sem=recv_sem,
        device_id=where,
        device_id_type=MESH,
    )


def drain(ref, sem):
    pltpu.make_async_copy(ref, ref, sem).wait()


def copy_here(src, dst, sem):
    copy = pltpu.make_async_copy(src, dst, sem)
    copy.start()
    return copy


class Ring:
    def __init__(self, count, own, slot, send_sem, recv_sem):
        self.count = count
        self.place = ring_position(lax.axis_index("ep"), count)
        self.far = count // 2
        self.near = count - 1 - self.far
        self.to = (ring_index(self.place + 1, count), ring_index(self.place - 1, count))
        self.own, self.slot = own, slot
        self.send_sem, self.recv_sem = send_sem, recv_sem
        self.hops = {}
        self.order = [
            (way, part)
            for turn in range(2)
            for pair in range(PARTS // 2)
            for way in range(2)
            for part in (2 * pair + (way + turn) % 2,)
        ]

    def reach(self, way, part):
        return self.far if way == part % 2 else self.near

    def origin(self, way, step):
        return ring_index(self.place - step if way == 0 else self.place + step, self.count)

    def hop(self, way, step, part):
        if step > self.reach(way, part):
            return
        block = self.origin(way, step - 1)
        self.hops[way, step, part] = remote(
            self.own(part) if step == 1 else self.slot(block, part),
            self.slot(block, part),
            self.send_sem,
            self.recv_sem.at[way, step - 1, part],
            {"ep": self.to[way]},
        )
        self.hops[way, step, part].start()

    def launch(self):
        for way, part in self.order:
            self.hop(way, 1, part)

    def relay(self, step):
        for way, part in self.order:
            if step <= self.reach(way, part):
                self.hops[way, step, part].wait_recv()
                self.hop(way, step + 1, part)

def number_of(offset, count):
    far = count // 2
    offset = offset % count
    if offset > far:
        offset -= count
    if offset == 0:
        return 0
    if offset == far:
        return count - 1
    return -2 * offset - 1 if offset < 0 else 2 * offset


def offset_of(number, count):
    if number == count - 1:
        return count // 2
    step = (number + 1) // 2
    return -step if number % 2 else step


class Pieces:
    def __init__(self, count, held, ring_send, ring_recv, side_send, side_recv):
        self.count = count
        self.place = ring_position(lax.axis_index("ep"), count)
        self.core = lax.axis_index("tp")
        self.far = count // 2
        self.near = count - 1 - self.far
        self.to = (ring_index(self.place + 1, count), ring_index(self.place - 1, count))
        self.held = held
        self.sems = (ring_send, ring_recv, side_send, side_recv)
        self.hops, self.sides = {}, {}

    def piece(self, offset, number):
        block = ring_index(self.place + offset + offset_of(number, self.count), self.count)
        return self.held.at[block, ring_index(self.place + offset, self.count), self.core]

    def reach(self, way, number):
        return self.far if number % 2 == way else self.near

    def hop(self, way, step, number):
        if step > self.reach(way, number):
            return
        ref = self.piece(-(step - 1) if way == 0 else step - 1, number)
        copy = remote(
            ref, ref, self.sems[0], self.sems[1].at[number, way, step - 1], {"ep": self.to[way]}
        )
        copy.start()
        self.hops[way, step, number] = copy

    def side(self, offset, number):
        ref = self.piece(offset, number)
        remote(ref, ref, self.sems[2], self.sems[3].at[offset % self.count], {"tp": 1 - self.core}).start()

    def launch(self, number):
        for turn in range(2):
            self.hop((number + turn) % 2, 1, number)
        self.side(0, number)

    def relay(self, step, number):
        for turn in range(2):
            way = (number + turn) % 2
            if step <= self.reach(way, number):
                self.hops[way, step, number].wait_recv()
                self.hop(way, step + 1, number)
                self.side(-step if way == 0 else step, number)

    def settle(self, offset):
        drain(self.held.at[0, :, 0], self.sems[3].at[offset % self.count])

    def finish(self):
        drain(self.held.at[: self.count - 1, :, 0], self.sems[0])
        drain(self.held.at[:, :, 0], self.sems[2])


def group_of(step, count):
    far = count // 2
    if step == 0:
        return [0]
    if step == far:
        return [count - 1]
    return [2 * step - 1, 2 * step]


ROWS = 256
PARTS = 4


def layer_kernel(
    count, ids_ref, visible_ref, request_ref, gain_ref, queries_hbm, cache_hbm, value_hbm, proj_hbm, residual_hbm, router_hbm,
    gate_hbm, up_hbm, down_hbm, hidden_ref, out_ref,
    queries, cache, values, proj, residual_own, residual, router, gate, up, down,
    limits, context, heads_own, heads_all, mine, theirs, held, ids_all, ids_row, hits, squares, logits_v, excited, mixing, active,
    sums, sums2, outbox, inbox, outbox2, inbox2, totals,
    load_sem, excite_sem, lower_sem, swap_sem, id_sem, res_sem,
    value_send, value_recv, heads_send, heads_recv, pair_send, pair_recv,
    piece_send, piece_recv, side_send, side_recv,
    both_send, both_recv, cross_send, cross_recv, back_send, back_recv,
):
    me = lax.axis_index("ep")
    core = lax.axis_index("tp")
    f32, bf16 = jnp.float32, jnp.bfloat16
    heads, _, latent, vdim = values.shape[0], values.shape[1], values.shape[1] * values.shape[2], values.shape[3]
    tokens = heads_own.shape[0]
    model = residual_own.shape[1]
    width = proj.shape[1]
    part = width // 2
    requests, columns, positions = cache.shape[1:]
    local = EXPERTS // count
    blocks = gate.shape[0] // local
    some = heads // PARTS
    half = tokens // PARTS
    place = ring_position(me, count)
    far = count // 2

    load_value = copy_here(value_hbm, values.at[:, me], load_sem.at[0])
    load_cache = copy_here(cache_hbm, cache.at[core], load_sem.at[1])
    load_residual = copy_here(residual_hbm, residual_own, load_sem.at[2])
    load_queries = copy_here(queries_hbm, queries, load_sem.at[3])
    load_proj = copy_here(proj_hbm, proj, load_sem.at[4])
    load_router = copy_here(router_hbm, router, load_sem.at[5])
    ids_all[me, :TOPK, :tokens] = ids_ref[...]
    greet(count)

    load_value.wait()
    value_ring = Ring(
        count,
        lambda p: values.at[pl.ds(p * some, some), me],
        lambda block, p: values.at[pl.ds(p * some, some), block],
        value_send, value_recv,
    )
    value_ring.launch()
    load_cache.wait()
    swap = remote(cache.at[core], cache.at[core], swap_sem.at[0], swap_sem.at[1], {"tp": 1 - core})
    swap.start()
    load_residual.wait()
    load_queries.wait()
    load_proj.wait()
    load_router.wait()
    for expert in range(local):
        span = pl.ds(expert * blocks, blocks)
        for source, target in ((gate_hbm, gate), (up_hbm, up)):
            pltpu.make_async_copy(source.at[span], target.at[span], excite_sem.at[expert]).start()
    load_down = copy_here(down_hbm, down, lower_sem)
    spreads = []
    for step in range(1, count):
        peer = lax.rem(me + step, count)
        column = pl.multiple_of(peer * width + core * part, part)
        spreads.append(
            remote(residual_own.at[:, pl.ds(column, part)], residual.at[me], res_sem.at[0], res_sem.at[1], {"ep": peer})
        )
        spreads.append(remote(ids_all.at[me], ids_all.at[me], id_sem.at[0], id_sem.at[1], {"ep": peer}))
    residual[me] = residual_own[:, pl.ds(pl.multiple_of(me * width + core * part, part), part)]

    visible, request = visible_ref[...], request_ref[...]
    row_token = lax.broadcasted_iota(jnp.int32, (tokens * heads, tokens), 0) // heads
    own_token = row_token == lax.broadcasted_iota(jnp.int32, (tokens * heads, tokens), 1)
    for r in range(requests):
        seen = jnp.where(request == r, visible, 0).astype(f32)
        limits[:, r : r + 1] = jnp.sum(jnp.where(own_token, seen, 0.0), axis=1, keepdims=True)

    def attend(start):
        rows = pl.ds(start, ROWS)
        asked = queries[rows, :]
        lane = lax.broadcasted_iota(jnp.int32, (ROWS, positions), 1).astype(f32)
        scored = []
        peak = None
        for r in range(requests):
            limit = limits[rows, r : r + 1]
            for side in range(2):
                score = jnp.dot(asked, cache[side, r], preferred_element_type=f32) * score_scale
                score = jnp.where(lane + float(side * positions) < limit, score, -jnp.inf)
                scored.append(score)
                top = jnp.max(score, axis=1, keepdims=True)
                peak = top if peak is None else jnp.maximum(peak, top)
        total, summed = None, None
        for number, score in enumerate(scored):
            weight = jnp.exp(score - peak).astype(bf16)
            amount = jnp.sum(weight.astype(f32), axis=1, keepdims=True)
            r, side = number // 2, number % 2
            term = lax.dot_general(
                weight, cache[side, r, :latent, :], (((1,), (1,)), ((), ())), preferred_element_type=f32
            )
            total = amount if total is None else total + amount
            summed = term if summed is None else summed + term
        summed = summed / total
        for piece in range(latent // 128):
            context[piece, rows, :] = summed[:, piece * 128 : (piece + 1) * 128]

    value_ring.relay(1)
    swap.wait_recv()
    chunks = list(range(0, tokens * heads, ROWS))
    done = 0
    for step in range(2, far + 1):
        until = -(-len(chunks) * (step - 1) // (far - 1)) if step < far else len(chunks)
        for start in chunks[done:until]:
            attend(start)
        done = until
        value_ring.relay(step)
        if step == 2:
            for copy in spreads:
                copy.start()
    for h in range(heads):
        rows = jnp.concatenate(
            [context[piece, pl.ds(h, tokens, stride=heads), :] for piece in range(latent // 128)], axis=1
        ).astype(bf16)
        heads_own[:, h * vdim : (h + 1) * vdim] = jnp.dot(
            rows, values[h].reshape(latent, vdim), preferred_element_type=f32
        ).astype(bf16)

    heads_ring = Ring(
        count,
        lambda p: heads_own.at[pl.ds(p * half, half)],
        lambda block, p: heads_all.at[block, pl.ds(p * half, half)],
        heads_send, heads_recv,
    )
    heads_ring.launch()
    pieces = Pieces(count, held, piece_send, piece_recv, side_send, side_recv)
    pairs = {}

    def block_at(offset):
        return ring_index(place + offset, count)

    def project(number):
        rows = heads_own[...] if number == 0 else heads_all[block_at(offset_of(number, count))]
        product = jnp.dot(rows, proj[...], preferred_element_type=f32)
        mine[number, 0] = product[:, :part]
        mine[number, 1] = product[:, part:]
        copy = remote(
            mine.at[number, 1 - core], theirs.at[number], pair_send, pair_recv.at[number],
            {"tp": 1 - core},
        )
        copy.start()
        pairs[number] = copy

    def conclude(number):
        if number == 0:
            drain(residual.at[: count - 1], res_sem.at[1])
            drain(ids_all.at[: count - 1], id_sem.at[1])
        pairs[number].wait_recv()
        block = block_at(offset_of(number, count))
        attention = mine[number, core] + theirs[number]
        held[block, me, core] = (residual[block].astype(f32) + attention).astype(bf16)
        pieces.launch(number)

    around = [offset if offset <= far else offset - count for offset in range(count)]
    dims = (((1,), (1,)), ((), ()))
    inner = blocks * gate.shape[1]

    def place_slots():
        before = (
            lax.broadcasted_iota(jnp.int32, (tokens, tokens), 0)
            < lax.broadcasted_iota(jnp.int32, (tokens, tokens), 1)
        ).astype(bf16)
        ids = [ids_all[block_at(offset)][:, :tokens] for offset in around]
        ids_row[...] = jnp.concatenate(ids, axis=1)
        expert = lax.broadcasted_iota(jnp.int32, (local, tokens), 0) + me * local
        here = []
        for one in ids:
            named = expert == one[0:1]
            for k in range(1, TOPK):
                named = named | (expert == one[k : k + 1])
            here.append(named.astype(f32))
        here = jnp.concatenate(here, axis=0)
        rank = jnp.dot(here.astype(bf16), before, preferred_element_type=f32)
        slot = lax.broadcasted_iota(jnp.int32, (count * local, CAP, tokens), 1).astype(f32)
        hit = (here[:, None, :] > 0.5) & (rank[:, None, :] == slot)
        hits[...] = jnp.where(hit, 1.0, 0.0).reshape(count, local * CAP, tokens).astype(bf16)

    def contract(offset):
        pieces.settle(offset)
        owner = block_at(offset)
        column = pl.ds(pl.multiple_of(owner * width, width), width)
        gain = gain_ref[pl.ds(owner, 1), :]
        first = offset == 0
        scaled, chosen = [], []
        for index, other in enumerate(around):
            span = pl.ds(index * tokens, tokens)
            block = block_at(other)
            sides = [held[block, owner, c].astype(f32) for c in range(2)]
            square = sides[0] * sides[0] + sides[1] * sides[1]
            squares[span, :] = square if first else squares[span, :] + square
            wide = (jnp.concatenate(sides, axis=1) * gain).astype(bf16)
            scaled.append(wide)
            chosen.append(jnp.dot(hits[index], wide, preferred_element_type=f32))
        part_logits = lax.dot_general(
            router[:, column], jnp.concatenate(scaled, axis=0), dims, preferred_element_type=f32
        )
        logits_v[...] = part_logits if first else logits_v[...] + part_logits
        for expert in range(local):
            if first:
                drain(gate.at[: 2 * blocks], excite_sem.at[expert])
            slots = jnp.concatenate(
                [one[expert * CAP : (expert + 1) * CAP] for one in chosen], axis=0
            ).astype(bf16)
            span = pl.ds(expert * blocks, blocks)
            for number, weight in enumerate((gate, up)):
                term = lax.dot_general(
                    weight[span, :, column].reshape(inner, width), slots, dims, preferred_element_type=f32
                )
                rows = pl.ds(number * inner, inner)
                excited[expert, rows, :] = term if first else excited[expert, rows, :] + term

    def activate():
        mean = jnp.sum(squares[...], axis=1, keepdims=True) / model
        scale = jnp.broadcast_to(lax.rsqrt(mean + epsilon), squares.shape).T[:1]
        lane = lax.broadcasted_iota(jnp.int32, (count * CAP, 128), 1)
        slot_scale = jnp.zeros((count * CAP, 128), f32)
        slot_scales = [
            jnp.sum(hits[index].astype(f32) * scale[:, index * tokens : (index + 1) * tokens], axis=1, keepdims=True)
            for index in range(count)
        ]
        for expert in range(local):
            own = jnp.concatenate([one[expert * CAP : (expert + 1) * CAP] for one in slot_scales], axis=0)
            slot_scale = jnp.where(lane == expert, own, slot_scale)
        slot_scale = slot_scale.T
        for expert in range(local):
            row = slot_scale[expert : expert + 1]
            gate_t = excited[expert, :inner, :] * row
            up_t = excited[expert, inner:, :] * row
            active[expert] = (gate_t / (1.0 + jnp.exp(-gate_t)) * up_t).T.astype(bf16)
        expert_row = lax.broadcasted_iota(jnp.int32, (EXPERTS, count * tokens), 0)
        named = expert_row == ids_row[0:1, :]
        for k in range(1, TOPK):
            named = named | (expert_row == ids_row[k : k + 1, :])
        logits = jnp.where(named, logits_v[...] * scale, -jnp.inf)
        raised = jnp.exp(logits - jnp.max(logits, axis=0, keepdims=True))
        logits_v[...] = raised / jnp.sum(raised, axis=0, keepdims=True)
        share = logits_v[pl.ds(pl.multiple_of(me * local, local), local), :].astype(bf16).astype(f32)
        for index in range(count):
            own = share[:, None, index * tokens : (index + 1) * tokens]
            own = jnp.broadcast_to(own, (local, CAP, tokens)).reshape(local * CAP, tokens)
            mixing[index] = (hits[index].astype(f32) * own).T.astype(bf16)

    due = {far: [0], far + 1: [1]}
    for distance in range(2, far):
        due[far + distance] = [1 - distance, distance]
    due[2 * far] = [1 - far, far]
    for turn in range(2 * far + 1):
        if 1 <= turn <= far:
            heads_ring.relay(turn)
        if turn <= far:
            for number in group_of(turn, count):
                project(number)
        for group in range(far + 1):
            if 1 <= turn - group <= far:
                for number in group_of(group, count):
                    pieces.relay(turn - group, number)
        if turn <= far:
            for number in group_of(turn, count):
                conclude(number)
        if turn == 0:
            place_slots()
        for offset in due.get(turn, ()):
            contract(offset)
    activate()

    hidden_ref[...] = jnp.concatenate(
        [held[me, (count // 2) * core + e, c] for e in range(count // 2) for c in range(2)], axis=1
    )

    load_down.wait()

    piece = sums.shape[4]
    turns = sums.shape[0]
    side_width = model // 2
    twin = me + 1 - 2 * lax.rem(me, 2)
    pair = count // 2
    steps = list(range(1, pair)) + [0]
    near_order = [lax.rem(me + 2 * step, count) for step in steps]
    twin_order = [lax.rem(twin + 2 * step, count) for step in steps]
    boths, crosses = {}, {}

    def lower(turn):
        rows = []
        for expert in range(local):
            span = pl.ds(expert * blocks, blocks)
            sides = [
                jnp.dot(
                    active[expert],
                    down[span, :, pl.ds(c * side_width + turn * piece, piece)].reshape(inner, piece),
                    preferred_element_type=f32,
                )
                for c in range(2)
            ]
            rows.append(jnp.concatenate(sides, axis=1))
        for offset in range(count):
            mine_rows = [row[offset * CAP : (offset + 1) * CAP] for row in rows]
            mixed = jnp.dot(
                mixing[offset], jnp.concatenate(mine_rows, axis=0).astype(bf16), preferred_element_type=f32
            ).astype(bf16)
            block = block_at(offset)
            for c in range(2):
                sums[turn, c, block] = mixed[:, c * piece : (c + 1) * piece]
        boths[turn] = remote(
            sums.at[turn, 1 - core], sums2.at[turn], both_send, both_recv.at[turn],
            {"tp": 1 - core},
        )
        boths[turn].start()

    def added(turn, block):
        return sums[turn, core, block].astype(f32) + sums2[turn, block].astype(f32)

    def cross(turn):
        boths[turn].wait_recv()
        for i, block in enumerate(twin_order):
            outbox[turn, i] = added(turn, block).astype(bf16)
        crosses[turn] = remote(
            outbox.at[turn], inbox.at[turn], cross_send, cross_recv.at[turn], {"ep": twin}
        )
        crosses[turn].start()

    def back(turn):
        crosses[turn].wait_recv()
        for i, block in enumerate(near_order):
            total = added(turn, block) + inbox[turn, i].astype(f32)
            if i == pair - 1:
                totals[turn] = total
                continue
            outbox2[turn, i] = total.astype(bf16)
            remote(
                outbox2.at[turn, i], inbox2.at[turn, i], back_send, back_recv.at[turn], {"ep": block}
            ).start()

    def end(turn):
        total = totals[turn]
        drain(inbox2.at[turn], back_recv.at[turn])
        for i in range(pair - 1):
            total = total + inbox2[turn, i].astype(f32)
        out_ref[:, turn * piece : (turn + 1) * piece] = total.astype(bf16)

    for turn in range(turns + 3):
        if turn < turns:
            lower(turn)
        if 1 <= turn <= turns:
            cross(turn - 1)
        if turn >= 3:
            back(turn - 3)
    for turn in range(turns):
        end(turn)

    drain(values.at[:, : count - 1], value_send)
    drain(heads_all.at[: count - 1], heads_send)
    pieces.finish()
    swap.wait_send()
    drain(residual.at[: count - 1], res_sem.at[0])
    drain(ids_all.at[: count - 1], id_sem.at[0])
    drain(theirs, pair_send)
    drain(sums2, both_send)
    drain(inbox, cross_send)
    drain(inbox2, back_send)


def dma(*shape):
    return pltpu.SemaphoreType.DMA(shape)


TURNS = 8


def lean_body(
    queries,
    latent_cache,
    residual,
    token_request,
    token_visible,
    value_proj,
    out_proj,
    norm_gain,
    router,
    expert_ids,
    gate_weight,
    up_weight,
    down_weight,
):
    count = lax.axis_size("ep")
    tokens, heads, columns = queries.shape
    requests, positions, _ = latent_cache.shape
    model = residual.shape[1]
    bf16, f32 = jnp.bfloat16, jnp.float32
    shape = jax.ShapeDtypeStruct
    far = count // 2
    local = EXPERTS // count
    width = out_proj.shape[1]
    slots = count * CAP
    blocks = gate_weight.shape[0] // local
    hidden_here = gate_weight.shape[2]
    piece = model // 2 // TURNS
    whole = pl.BlockSpec(memory_space=pltpu.VMEM)
    anywhere = pl.BlockSpec(memory_space=pl.ANY)
    vmem = pltpu.VMEM
    weight = (gate_weight.shape[0], hidden_here, model)
    hidden, expert_out = pl.pallas_call(
        functools.partial(layer_kernel, count),
        out_shape=(shape((tokens, model // 2), bf16), shape((tokens, model // 2), bf16)),
        in_specs=[whole] * 4 + [anywhere] * 9,
        out_specs=(whole, whole),
        scratch_shapes=[
            vmem((tokens * heads, columns), bf16),
            vmem((2, requests, columns, positions), bf16),
            vmem((heads, count) + value_proj.shape[1:], bf16),
            vmem(out_proj.shape, bf16),
            vmem((tokens, model), bf16),
            vmem((count, tokens, width // 2), bf16),
            vmem((EXPERTS, model), bf16),
            vmem(weight, bf16),
            vmem(weight, bf16),
            vmem(weight, bf16),
            vmem((tokens * heads, 128), f32),
            vmem((LATENT // 128, tokens * heads, 128), f32),
            vmem((tokens, heads * VDIM), bf16),
            vmem((count, tokens, heads * VDIM), bf16),
            vmem((count, 2, tokens, width // 2), f32),
            vmem((count, tokens, width // 2), f32),
            vmem((count, count, 2, tokens, width // 2), bf16),
            vmem((count, 8, 128), jnp.int32),
            vmem((8, count * tokens), jnp.int32),
            vmem((count, local * CAP, tokens), bf16),
            vmem((count * tokens, 128), f32),
            vmem((EXPERTS, count * tokens), f32),
            vmem((local, 2 * blocks * hidden_here, slots), f32),
            vmem((count, tokens, local * CAP), bf16),
            vmem((local, slots, blocks * hidden_here), bf16),
            vmem((TURNS, 2, count, tokens, piece), bf16),
            vmem((TURNS, count, tokens, piece), bf16),
            vmem((TURNS, far, tokens, piece), bf16),
            vmem((TURNS, far, tokens, piece), bf16),
            vmem((TURNS, far - 1, tokens, piece), bf16),
            vmem((TURNS, far - 1, tokens, piece), bf16),
            vmem((TURNS, tokens, piece), f32),
            dma(6), dma(local), dma(), dma(2), dma(2), dma(2),
            dma(), dma(2, far, PARTS), dma(), dma(2, far, PARTS), dma(), dma(count),
            dma(), dma(count, 2, far), dma(), dma(count),
            dma(), dma(TURNS), dma(), dma(TURNS), dma(), dma(TURNS),
        ],
        compiler_params=pltpu.CompilerParams(
            collective_id=0, has_side_effects=True, vmem_limit_bytes=59 * 2**20
        ),
    )(
        expert_ids.T, token_visible[None], token_request[None], norm_gain.reshape(count, model // count), queries.reshape(tokens * heads, columns),
        jnp.swapaxes(latent_cache, 1, 2), value_proj, out_proj, residual, router.T,
        jnp.swapaxes(gate_weight, 1, 2), jnp.swapaxes(up_weight, 1, 2), down_weight,
    )
    return (hidden, expert_out)


LEAN_BYTES = 8 * 2**20


def choose(mesh):
    count = mesh.shape["ep"]

    def layer(*args):
        tokens, model = args[2].shape
        fits = count * tokens * model * 2 <= LEAN_BYTES
        even = count % 2 == 0 and count >= 4 and tokens % 32 == 0 and EXPERTS % count == 0
        if fits and even and mesh.shape["tp"] == 2:
            return lean_body(*args)
        return body(*args)

    return layer


def solution(mesh):
    return jax.shard_map(
        choose(mesh),
        mesh=mesh,
        in_specs=(
            P(("grp", "ep"), "tp", None),
            P(("grp", "ep"), "tp", None),
            P(("grp", "ep"), None),
            P(("grp", "ep")),
            P(("grp", "ep")),
            P("tp", "ep", None),
            P("tp", "ep"),
            P(),
            P(),
            P(("grp", "ep"), None),
            P("ep", None, "tp"),
            P("ep", None, "tp"),
            P("ep", "tp", None),
        ),
        out_specs=(P(("grp", "ep"), "tp"), P(("grp", "ep"), "tp")),
        check_vma=False,
    )
```

```python
import functools

import jax
import jax.numpy as jnp
from jax import lax
from jax.experimental import pallas as pl
from jax.experimental.pallas import tpu as pltpu
from jax.sharding import PartitionSpec as P

LATENT = 512
VDIM = 128
EXPERTS = 64
TOPK = 6
GROUPS = 2
CAP = 8
PIECES = 128
MESH = pl.DeviceIdType.MESH


score_scale = 192.0 ** (-0.5)
epsilon = 1e-06


def masked_scores(queries, block_rows, token_request, token_visible):
    per_request = block_rows.shape[1]
    flat_rows = block_rows.reshape(-1, block_rows.shape[2])
    scores = (
        jnp.einsum("thc,kc->thk", queries, flat_rows, preferred_element_type=jnp.float32)
        * score_scale
    )
    column = jnp.arange(flat_rows.shape[0], dtype=jnp.int32)
    owner_id = column // per_request
    position = column % per_request
    allowed = (owner_id[None, :] == token_request[:, None]) & (
        position[None, :] < token_visible[:, None]
    )
    return (jnp.where(allowed[:, None, :], scores, -jnp.inf), flat_rows)


def weighted_rows(scores, row_peak, flat_rows):
    weights = jnp.exp(scores - row_peak[:, :, None]).astype(jnp.bfloat16)
    totals = jnp.sum(weights.astype(jnp.float32), axis=2)
    summed = jnp.einsum(
        "thk,kc->thc", weights, flat_rows[:, :LATENT], preferred_element_type=jnp.float32
    )
    return (summed, totals)


def expert_block(arrived, gate_weight, up_weight, down_weight):
    gate_vals = jnp.einsum("prd,pdf->prf", arrived, gate_weight, preferred_element_type=jnp.float32)
    up_vals = jnp.einsum("prd,pdf->prf", arrived, up_weight, preferred_element_type=jnp.float32)
    activated = (jax.nn.silu(gate_vals) * up_vals).astype(jnp.bfloat16)
    return jnp.einsum(
        "prf,pfd->prd", activated, down_weight, preferred_element_type=jnp.float32
    ).astype(jnp.bfloat16)


def body(
    queries,
    latent_cache,
    residual,
    token_request,
    token_visible,
    value_proj,
    out_proj,
    norm_gain,
    router,
    expert_ids,
    gate_weight,
    up_weight,
    down_weight,
):
    all_rows = lax.all_gather(latent_cache, "tp", axis=1, tiled=True)
    scores, flat_rows = masked_scores(queries, all_rows, token_request, token_visible)
    summed, totals = weighted_rows(scores, jnp.max(scores, axis=2), flat_rows)
    context = (summed / totals[:, :, None]).astype(jnp.bfloat16)
    tokens_here = context.shape[0]
    heads_here = context.shape[1]
    head_values = jnp.einsum(
        "thl,hlv->thv",
        context,
        lax.all_gather(value_proj, "ep", axis=1, tiled=True),
        preferred_element_type=jnp.float32,
    )
    heads_out = head_values.astype(jnp.bfloat16).reshape(tokens_here, heads_here * VDIM)
    column_block = jnp.dot(
        lax.all_gather(heads_out, "ep", axis=0, tiled=True),
        out_proj,
        preferred_element_type=jnp.float32,
    )
    attention_part = lax.all_to_all(column_block, "ep", split_axis=0, concat_axis=1, tiled=True)
    attention = lax.psum(attention_part, "tp")
    hidden = (residual.astype(jnp.float32) + attention).astype(jnp.bfloat16)
    hidden_wide = hidden.astype(jnp.float32)
    normed = (
        hidden_wide
        * lax.rsqrt(jnp.mean(hidden_wide * hidden_wide, axis=1, keepdims=True) + epsilon)
        * norm_gain
    ).astype(jnp.bfloat16)
    logits = jnp.dot(normed, router, preferred_element_type=jnp.float32)
    gate_share = jax.nn.softmax(jnp.take_along_axis(logits, expert_ids, axis=1), axis=1).astype(
        jnp.bfloat16
    )
    flat_ids = expert_ids.reshape(-1)
    position_id = jnp.arange(flat_ids.shape[0], dtype=jnp.int32)
    earlier = (flat_ids[:, None] == flat_ids[None, :]) & (
        position_id[None, :] < position_id[:, None]
    )
    slot_ids = (flat_ids * CAP + jnp.sum(earlier.astype(jnp.int32), axis=1)).reshape(
        tokens_here, TOPK
    )
    targets = jnp.arange(EXPERTS * CAP, dtype=jnp.int32)
    matches = slot_ids[:, :, None] == targets[None, None, :]
    picker = jnp.any(matches, axis=1).T.astype(jnp.bfloat16)
    model_width = normed.shape[1]
    mixing = jnp.sum(
        jnp.where(matches, gate_share[:, :, None], jnp.zeros((), jnp.bfloat16)), axis=1
    )
    mixing = jnp.broadcast_to(
        mixing.reshape(tokens_here, EXPERTS, 1, CAP), (tokens_here, EXPERTS, GROUPS, CAP)
    ).reshape(tokens_here, PIECES * CAP)
    core_count = lax.axis_size("tp")
    half_width = model_width // core_count
    core_start = lax.axis_index("tp") * half_width
    outgoing = jnp.dot(picker, normed, preferred_element_type=jnp.float32).astype(jnp.bfloat16)
    outgoing = jnp.broadcast_to(
        outgoing.reshape(EXPERTS, 1, CAP, model_width), (EXPERTS, GROUPS, CAP, model_width)
    ).reshape(PIECES, CAP, model_width)
    arrived = lax.all_to_all(outgoing, "ep", split_axis=0, concat_axis=1, tiled=True)
    partial_out = expert_block(arrived, gate_weight, up_weight, down_weight)
    returned = lax.all_to_all(partial_out, "ep", split_axis=1, concat_axis=0, tiled=True)
    routed = jnp.dot(
        mixing, returned.reshape(PIECES * CAP, model_width), preferred_element_type=jnp.float32
    )
    expert_out = lax.psum_scatter(
        routed.astype(jnp.bfloat16), "tp", scatter_dimension=1, tiled=True
    )
    hidden_part = lax.dynamic_slice_in_dim(hidden, core_start, half_width, 1)
    return (hidden_part, expert_out)


def ring_position(index, count):
    half = lax.div(index, 2)
    return half + lax.rem(index, 2) * (count - 1 - 2 * half)


def ring_index(place, count):
    place = lax.rem(place + count, count)
    upper = lax.div(place, count // 2)
    return 2 * place + upper * (2 * count - 1 - 4 * place)


def greet(count):
    me = lax.axis_index("ep")
    core = lax.axis_index("tp")
    barrier = pltpu.get_barrier_semaphore()
    for step in range(1, count):
        pl.semaphore_signal(
            barrier, inc=1, device_id={"ep": lax.rem(me + step, count)}, device_id_type=MESH
        )
    pl.semaphore_signal(barrier, inc=1, device_id={"tp": 1 - core}, device_id_type=MESH)
    pl.semaphore_wait(barrier, count)


def remote(src, dst, send_sem, recv_sem, where):
    return pltpu.make_async_remote_copy(
        src_ref=src,
        dst_ref=dst,
        send_sem=send_sem,
        recv_sem=recv_sem,
        device_id=where,
        device_id_type=MESH,
    )


def drain(ref, sem):
    pltpu.make_async_copy(ref, ref, sem).wait()


def copy_here(src, dst, sem):
    copy = pltpu.make_async_copy(src, dst, sem)
    copy.start()
    return copy


class Ring:
    def __init__(self, count, own, slot, send_sem, recv_sem):
        self.count = count
        self.place = ring_position(lax.axis_index("ep"), count)
        self.far = count // 2
        self.near = count - 1 - self.far
        self.to = (ring_index(self.place + 1, count), ring_index(self.place - 1, count))
        self.own, self.slot = own, slot
        self.send_sem, self.recv_sem = send_sem, recv_sem
        self.hops = {}
        self.order = [
            (way, part)
            for turn in range(2)
            for pair in range(PARTS // 2)
            for way in range(2)
            for part in (2 * pair + (way + turn) % 2,)
        ]

    def reach(self, way, part):
        return self.far if way == part % 2 else self.near

    def origin(self, way, step):
        return ring_index(self.place - step if way == 0 else self.place + step, self.count)

    def hop(self, way, step, part):
        if step > self.reach(way, part):
            return
        block = self.origin(way, step - 1)
        self.hops[way, step, part] = remote(
            self.own(part) if step == 1 else self.slot(block, part),
            self.slot(block, part),
            self.send_sem,
            self.recv_sem.at[way, step - 1, part],
            {"ep": self.to[way]},
        )
        self.hops[way, step, part].start()

    def launch(self):
        for way, part in self.order:
            self.hop(way, 1, part)

    def relay(self, step):
        for way, part in self.order:
            if step <= self.reach(way, part):
                self.hops[way, step, part].wait_recv()
                self.hop(way, step + 1, part)

def number_of(offset, count):
    far = count // 2
    offset = offset % count
    if offset > far:
        offset -= count
    if offset == 0:
        return 0
    if offset == far:
        return count - 1
    return -2 * offset - 1 if offset < 0 else 2 * offset


def offset_of(number, count):
    if number == count - 1:
        return count // 2
    step = (number + 1) // 2
    return -step if number % 2 else step


class Pieces:
    def __init__(self, count, held, ring_send, ring_recv, side_send, side_recv):
        self.count = count
        self.place = ring_position(lax.axis_index("ep"), count)
        self.core = lax.axis_index("tp")
        self.far = count // 2
        self.near = count - 1 - self.far
        self.to = (ring_index(self.place + 1, count), ring_index(self.place - 1, count))
        self.held = held
        self.sems = (ring_send, ring_recv, side_send, side_recv)
        self.hops, self.sides = {}, {}

    def piece(self, offset, number):
        block = ring_index(self.place + offset + offset_of(number, self.count), self.count)
        return self.held.at[block, ring_index(self.place + offset, self.count), self.core]

    def reach(self, way, number):
        return self.far if number % 2 == way else self.near

    def hop(self, way, step, number):
        if step > self.reach(way, number):
            return
        ref = self.piece(-(step - 1) if way == 0 else step - 1, number)
        copy = remote(
            ref, ref, self.sems[0], self.sems[1].at[number, way, step - 1], {"ep": self.to[way]}
        )
        copy.start()
        self.hops[way, step, number] = copy

    def side(self, offset, number):
        ref = self.piece(offset, number)
        remote(ref, ref, self.sems[2], self.sems[3].at[offset % self.count], {"tp": 1 - self.core}).start()

    def launch(self, number):
        for turn in range(2):
            self.hop((number + turn) % 2, 1, number)
        self.side(0, number)

    def relay(self, step, number):
        for turn in range(2):
            way = (number + turn) % 2
            if step <= self.reach(way, number):
                self.hops[way, step, number].wait_recv()
                self.hop(way, step + 1, number)
                self.side(-step if way == 0 else step, number)

    def settle(self, offset):
        drain(self.held.at[0, :, 0], self.sems[3].at[offset % self.count])

    def finish(self):
        drain(self.held.at[: self.count - 1, :, 0], self.sems[0])
        drain(self.held.at[:, :, 0], self.sems[2])


def group_of(step, count):
    far = count // 2
    if step == 0:
        return [0]
    if step == far:
        return [count - 1]
    return [2 * step - 1, 2 * step]


ROWS = 256
PARTS = 4


def layer_kernel(
    count, ids_hbm, visible_hbm, request_hbm, gain_hbm, queries_hbm, cache_hbm, value_hbm, proj_hbm, residual_hbm, router_hbm,
    gate_hbm, up_hbm, down_hbm, hidden_hbm, out_hbm,
    ids_ref, visible_ref, request_ref, gain_ref,
    queries, cache, values, proj, residual_own, residual, router, gate, up, down,
    limits, context, heads_own, heads_all, theirs, held, ids_all, ids_row, hits, logits_v, scales, excited, mixing, active,
    sums2, inbox, inbox2,
    load_sem, excite_sem, lower_sem, swap_sem, id_sem, res_sem,
    value_send, value_recv, heads_send, heads_recv, pair_send, pair_recv,
    piece_send, piece_recv, side_send, side_recv,
    both_send, both_recv, cross_send, cross_recv, back_send, back_recv, store_sem,
):
    me = lax.axis_index("ep")
    core = lax.axis_index("tp")
    f32, bf16 = jnp.float32, jnp.bfloat16
    heads, _, latent, vdim = values.shape[0], values.shape[1], values.shape[1] * values.shape[2], values.shape[3]
    tokens = heads_own.shape[0]
    model = residual_own.shape[1]
    width = proj.shape[1]
    part = width // 2
    requests, columns, positions = cache.shape[1:]
    local = EXPERTS // count
    blocks = gate.shape[0] // local
    some = heads // PARTS
    half = tokens // PARTS
    place = ring_position(me, count)
    far = count // 2

    load_value = copy_here(value_hbm, values.at[:, me], load_sem.at[0])
    load_cache = copy_here(cache_hbm, cache.at[core], load_sem.at[1])
    load_small = [
        copy_here(source, target, load_sem.at[6 + number])
        for number, (source, target) in enumerate(
            ((ids_hbm, ids_ref), (visible_hbm, visible_ref), (request_hbm, request_ref), (gain_hbm, gain_ref))
        )
    ]
    load_residual = copy_here(residual_hbm, residual_own, load_sem.at[2])
    load_queries = copy_here(queries_hbm, queries, load_sem.at[3])
    load_proj = copy_here(proj_hbm, proj, load_sem.at[4])
    load_router = copy_here(router_hbm, router, load_sem.at[5])
    greet(count)

    load_value.wait()
    value_ring = Ring(
        count,
        lambda p: values.at[pl.ds(p * some, some), me],
        lambda block, p: values.at[pl.ds(p * some, some), block],
        value_send, value_recv,
    )
    value_ring.launch()
    for copy in load_small:
        copy.wait()
    ids_all[me, :TOPK, :tokens] = ids_ref[...]
    load_cache.wait()
    swap = remote(cache.at[core], cache.at[core], swap_sem.at[0], swap_sem.at[1], {"tp": 1 - core})
    swap.start()
    load_residual.wait()
    load_queries.wait()
    load_proj.wait()
    load_router.wait()
    for expert in range(local):
        span = pl.ds(expert * blocks, blocks)
        for source, target in ((gate_hbm, gate), (up_hbm, up)):
            pltpu.make_async_copy(source.at[span], target.at[span], excite_sem).start()
    load_down = copy_here(down_hbm, down, lower_sem)
    spreads = []
    for step in range(1, count):
        peer = lax.rem(me + step, count)
        column = pl.multiple_of(peer * width + core * part, part)
        spreads.append(
            remote(residual_own.at[:, pl.ds(column, part)], residual.at[me], res_sem.at[0], res_sem.at[1], {"ep": peer})
        )
        spreads.append(remote(ids_all.at[me], ids_all.at[me], id_sem.at[0], id_sem.at[1], {"ep": peer}))
    residual[me] = residual_own[:, pl.ds(pl.multiple_of(me * width + core * part, part), part)]

    visible, request = visible_ref[...], request_ref[...]
    row_token = lax.broadcasted_iota(jnp.int32, (tokens * heads, tokens), 0) // heads
    own_token = row_token == lax.broadcasted_iota(jnp.int32, (tokens * heads, tokens), 1)
    for r in range(requests):
        seen = jnp.where(request == r, visible, 0).astype(f32)
        limits[:, r : r + 1] = jnp.sum(jnp.where(own_token, seen, 0.0), axis=1, keepdims=True)

    def attend(start):
        rows = pl.ds(start, ROWS)
        asked = queries[rows, :]
        lane = lax.broadcasted_iota(jnp.int32, (ROWS, positions), 1).astype(f32)
        scored = []
        peak = None
        for r in range(requests):
            limit = limits[rows, r : r + 1]
            for side in range(2):
                score = jnp.dot(asked, cache[side, r], preferred_element_type=f32) * score_scale
                score = jnp.where(lane + float(side * positions) < limit, score, -jnp.inf)
                scored.append(score)
                top = jnp.max(score, axis=1, keepdims=True)
                peak = top if peak is None else jnp.maximum(peak, top)
        total, summed = None, None
        for number, score in enumerate(scored):
            weight = jnp.exp(score - peak).astype(bf16)
            amount = jnp.sum(weight.astype(f32), axis=1, keepdims=True)
            r, side = number // 2, number % 2
            term = lax.dot_general(
                weight, cache[side, r, :latent, :], (((1,), (1,)), ((), ())), preferred_element_type=f32
            )
            total = amount if total is None else total + amount
            summed = term if summed is None else summed + term
        summed = summed / total
        for piece in range(latent // 128):
            context[piece, rows, :] = summed[:, piece * 128 : (piece + 1) * 128]

    value_ring.relay(1)
    swap.wait_recv()
    chunks = list(range(0, tokens * heads, ROWS))
    done = 0
    for step in range(2, far + 1):
        until = -(-len(chunks) * (step - 1) // (far - 1)) if step < far else len(chunks)
        for start in chunks[done:until]:
            attend(start)
        done = until
        value_ring.relay(step)
        if step == 2:
            for copy in spreads:
                copy.start()
    for h in range(heads):
        rows = jnp.concatenate(
            [context[piece, pl.ds(h, tokens, stride=heads), :] for piece in range(latent // 128)], axis=1
        ).astype(bf16)
        heads_own[:, h * vdim : (h + 1) * vdim] = jnp.dot(
            rows, values[h].reshape(latent, vdim), preferred_element_type=f32
        ).astype(bf16)

    heads_ring = Ring(
        count,
        lambda p: heads_own.at[pl.ds(p * half, half)],
        lambda block, p: heads_all.at[block, pl.ds(p * half, half)],
        heads_send, heads_recv,
    )
    heads_ring.launch()
    mine = context
    pieces = Pieces(count, held, piece_send, piece_recv, side_send, side_recv)
    pairs = {}

    def block_at(offset):
        return ring_index(place + offset, count)

    def project(number):
        rows = heads_own[...] if number == 0 else heads_all[block_at(offset_of(number, count))]
        product = jnp.dot(rows, proj[...], preferred_element_type=f32)
        rows = pl.ds(number * tokens, tokens)
        mine[0, rows, :] = product[:, :part]
        mine[1, rows, :] = product[:, part:]
        copy = remote(
            mine.at[1 - core, rows, :], theirs.at[number], pair_send, pair_recv.at[number],
            {"tp": 1 - core},
        )
        copy.start()
        pairs[number] = copy

    def conclude(number):
        if number == 0:
            drain(residual.at[: count - 1], res_sem.at[1])
            drain(ids_all.at[: count - 1], id_sem.at[1])
        pairs[number].wait_recv()
        block = block_at(offset_of(number, count))
        attention = mine[core, pl.ds(number * tokens, tokens), :] + theirs[number]
        held[block, me, core] = (residual[block].astype(f32) + attention).astype(bf16)
        pieces.launch(number)

    squares = limits
    around = [offset if offset <= far else offset - count for offset in range(count)]
    dims = (((1,), (1,)), ((), ()))
    inner = blocks * gate.shape[1]

    def place_slots():
        before = (
            lax.broadcasted_iota(jnp.int32, (tokens, tokens), 0)
            < lax.broadcasted_iota(jnp.int32, (tokens, tokens), 1)
        ).astype(bf16)
        ids = [ids_all[block_at(offset)][:, :tokens] for offset in around]
        ids_row[...] = jnp.concatenate(ids, axis=1)
        expert = lax.broadcasted_iota(jnp.int32, (local, tokens), 0) + me * local
        here = []
        for one in ids:
            named = expert == one[0:1]
            for k in range(1, TOPK):
                named = named | (expert == one[k : k + 1])
            here.append(named.astype(f32))
        here = jnp.concatenate(here, axis=0)
        rank = jnp.dot(here.astype(bf16), before, preferred_element_type=f32)
        slot = lax.broadcasted_iota(jnp.int32, (count * local, CAP, tokens), 1).astype(f32)
        hit = (here[:, None, :] > 0.5) & (rank[:, None, :] == slot)
        hits[...] = jnp.where(hit, 1.0, 0.0).reshape(count, local * CAP, tokens).astype(bf16)

    def columns_of(offset):
        return pl.ds(pl.multiple_of(block_at(offset) * width, width), width)

    def prepare(offset):
        owner = block_at(offset)
        gain = gain_ref[:, columns_of(offset)]
        first = offset == 0
        scaled, chosen = [], []
        for index, other in enumerate(around):
            span = pl.ds(index * tokens, tokens)
            block = block_at(other)
            sides = [held[block, owner, c].astype(f32) for c in range(2)]
            square = sides[0] * sides[0] + sides[1] * sides[1]
            squares[span, :] = square if first else squares[span, :] + square
            wide = (jnp.concatenate(sides, axis=1) * gain).astype(bf16)
            scaled.append(wide)
            chosen.append(jnp.dot(hits[index], wide, preferred_element_type=f32))
        part_logits = lax.dot_general(
            router[:, columns_of(offset)], jnp.concatenate(scaled, axis=0), dims, preferred_element_type=f32
        )
        logits_v[...] = part_logits if first else logits_v[...] + part_logits
        return [
            jnp.concatenate(
                [one[expert * CAP : (expert + 1) * CAP] for one in chosen], axis=0
            ).astype(bf16)
            for expert in range(local)
        ]

    def stream(offset, slots):
        column = columns_of(offset)
        for expert in range(local):
            span = pl.ds(expert * blocks, blocks)
            weights = jnp.concatenate(
                [weight[span, :, column].reshape(inner, width) for weight in (gate, up)], axis=0
            )
            term = lax.dot_general(weights, slots[expert], dims, preferred_element_type=f32)
            excited[expert] = term if offset == 0 else excited[expert] + term

    def contract(offset, last=False):
        pieces.settle(offset)
        slots = prepare(offset)
        if last:
            weigh()
        stream(offset, slots)

    def weigh():
        mean = jnp.sum(squares[...], axis=1, keepdims=True) / model
        scale = jnp.broadcast_to(lax.rsqrt(mean + epsilon), squares.shape).T[:1]
        lane = lax.broadcasted_iota(jnp.int32, (count * CAP, 128), 1)
        slot_scale = jnp.zeros((count * CAP, 128), f32)
        slot_scales = [
            jnp.sum(hits[index].astype(f32) * scale[:, index * tokens : (index + 1) * tokens], axis=1, keepdims=True)
            for index in range(count)
        ]
        for expert in range(local):
            own = jnp.concatenate([one[expert * CAP : (expert + 1) * CAP] for one in slot_scales], axis=0)
            slot_scale = jnp.where(lane == expert, own, slot_scale)
        scales[...] = slot_scale.T[:local]
        expert_row = lax.broadcasted_iota(jnp.int32, (EXPERTS, count * tokens), 0)
        named = expert_row == ids_row[0:1, :]
        for k in range(1, TOPK):
            named = named | (expert_row == ids_row[k : k + 1, :])
        logits = jnp.where(named, logits_v[...] * scale, -jnp.inf)
        raised = jnp.exp(logits - jnp.max(logits, axis=0, keepdims=True))
        logits_v[...] = raised / jnp.sum(raised, axis=0, keepdims=True)
        share = logits_v[pl.ds(pl.multiple_of(me * local, local), local), :].astype(bf16).astype(f32)
        for index in range(count):
            own = share[:, None, index * tokens : (index + 1) * tokens]
            own = jnp.broadcast_to(own, (local, CAP, tokens)).reshape(local * CAP, tokens)
            mixing[index] = (hits[index].astype(f32) * own).T.astype(bf16)

    def activate():
        for expert in range(local):
            row = scales[expert : expert + 1]
            gate_t = excited[expert, :inner, :] * row
            up_t = excited[expert, inner:, :] * row
            active[expert] = (gate_t / (1.0 + jnp.exp(-gate_t)) * up_t).T.astype(bf16)

    due = {far: [0], far + 1: [1]}
    for distance in range(2, far):
        due[far + distance] = [1 - distance, distance]
    due[2 * far] = [1 - far, far]
    for turn in range(2 * far + 1):
        if turn == far:
            drain(gate, excite_sem)
            drain(up, excite_sem)
        if 1 <= turn <= far:
            heads_ring.relay(turn)
        if turn <= far:
            for number in group_of(turn, count):
                project(number)
        for group in range(far + 1):
            if 1 <= turn - group <= far:
                for number in group_of(group, count):
                    pieces.relay(turn - group, number)
        if turn <= far:
            for number in group_of(turn, count):
                conclude(number)
        if turn == 0:
            place_slots()
        for offset in due.get(turn, ()):
            contract(offset, offset == far)
    activate()

    for e in range(count // 2):
        for c in range(2):
            number = 2 * e + c
            copy_here(
                held.at[me, (count // 2) * core + e, c],
                hidden_hbm.at[:, pl.ds(number * part, part)],
                store_sem.at[0],
            )
    load_down.wait()

    turns = sums2.shape[0]
    piece = sums2.shape[2] // count
    sums = gate
    side_width = model // 2
    twin = me + 1 - 2 * lax.rem(me, 2)
    pair = count // 2
    steps = list(range(1, pair)) + [0]
    near_order = [lax.rem(me + 2 * step, count) for step in steps]
    twin_order = [lax.rem(twin + 2 * step, count) for step in steps]
    boths, crosses = {}, {}

    def lanes_of(block):
        return pl.ds(pl.multiple_of(block * piece, piece), piece)

    def lower(turn):
        rows = []
        for expert in range(local):
            span = pl.ds(expert * blocks, blocks)
            sides = [
                jnp.dot(
                    active[expert],
                    down[span, :, pl.ds(c * side_width + turn * piece, piece)].reshape(inner, piece),
                    preferred_element_type=f32,
                )
                for c in range(2)
            ]
            rows.append(jnp.concatenate(sides, axis=1))
        for offset in range(count):
            mine_rows = [row[offset * CAP : (offset + 1) * CAP] for row in rows]
            mixed = jnp.dot(
                mixing[offset], jnp.concatenate(mine_rows, axis=0).astype(bf16), preferred_element_type=f32
            ).astype(bf16)
            for c in range(2):
                sums[2 * turn + c, :tokens, lanes_of(block_at(offset))] = mixed[:, c * piece : (c + 1) * piece]
        boths[turn] = remote(
            sums.at[2 * turn + 1 - core, pl.ds(0, tokens), pl.ds(0, count * piece)], sums2.at[turn], both_send, both_recv.at[turn],
            {"tp": 1 - core},
        )
        boths[turn].start()

    def added(turn, block):
        own = sums[2 * turn + core, :tokens, lanes_of(block)]
        return own.astype(f32) + sums2[turn, :, lanes_of(block)].astype(f32)

    swap.wait_send()
    fits = columns // (pair * tokens)

    def outbox(which, turn, rows):
        at, lane = turn // (positions // piece), turn % (positions // piece)
        return cache.at[
            which, at // fits, pl.ds(at % fits * pair * tokens, rows), pl.ds(lane * piece, piece)
        ]

    def cross(turn):
        boths[turn].wait_recv()
        box = outbox(0, turn, pair * tokens)
        for i, block in enumerate(twin_order):
            box[i * tokens : (i + 1) * tokens, :] = added(turn, block).astype(bf16)
        crosses[turn] = remote(box, inbox.at[turn], cross_send, cross_recv.at[turn], {"ep": twin})
        crosses[turn].start()

    def back(turn):
        crosses[turn].wait_recv()
        box = outbox(1, turn, (pair - 1) * tokens)
        for i, block in enumerate(near_order):
            rows = pl.ds(i * tokens, tokens)
            total = added(turn, block) + inbox[turn, rows, :].astype(f32)
            if i == pair - 1:
                limits[turn * tokens : (turn + 1) * tokens, :piece] = total
                continue
            box[rows, :] = total.astype(bf16)
            remote(box.at[rows, :], inbox2.at[turn, i], back_send, back_recv.at[turn], {"ep": block}).start()

    def end(turn):
        total = limits[turn * tokens : (turn + 1) * tokens, :piece]
        drain(inbox2.at[turn], back_recv.at[turn])
        for i in range(pair - 1):
            total = total + inbox2[turn, i].astype(f32)
        span = pl.ds(turn * piece, piece)
        out_v[:, span] = total.astype(bf16)
        copy_here(out_v.at[:, span], out_hbm.at[:, span], store_sem.at[1])

    for turn in range(turns + 3):
        if turn < turns:
            lower(turn)
        if 1 <= turn <= turns:
            cross(turn - 1)
        if turn >= 3:
            back(turn - 3)
    drain(heads_all.at[: count - 1], heads_send)
    out_v = heads_own
    for turn in range(turns):
        end(turn)

    drain(values.at[:, : count - 1], value_send)
    pieces.finish()
    drain(residual.at[: count - 1], res_sem.at[0])
    drain(ids_all.at[: count - 1], id_sem.at[0])
    drain(theirs, pair_send)
    drain(sums2, both_send)
    drain(inbox, cross_send)
    drain(inbox2, back_send)
    drain(heads_own, store_sem.at[0])
    drain(heads_own, store_sem.at[1])


def store_kernel(hidden_hbm, out_hbm, hidden_to, out_to, hidden_v, out_v, in_sem, out_sem):
    loads = [copy_here(hidden_hbm, hidden_v, in_sem.at[0]), copy_here(out_hbm, out_v, in_sem.at[1])]
    loads[0].wait()
    stores = [copy_here(hidden_v, hidden_to, out_sem.at[0])]
    loads[1].wait()
    stores.append(copy_here(out_v, out_to, out_sem.at[1]))
    for copy in stores:
        copy.wait()


def dma(*shape):
    return pltpu.SemaphoreType.DMA(shape)


TURNS = 8


def lean_body(
    queries,
    latent_cache,
    residual,
    token_request,
    token_visible,
    value_proj,
    out_proj,
    norm_gain,
    router,
    expert_ids,
    gate_weight,
    up_weight,
    down_weight,
):
    count = lax.axis_size("ep")
    tokens, heads, columns = queries.shape
    requests, positions, _ = latent_cache.shape
    model = residual.shape[1]
    bf16, f32 = jnp.bfloat16, jnp.float32
    shape = jax.ShapeDtypeStruct
    far = count // 2
    local = EXPERTS // count
    width = out_proj.shape[1]
    slots = count * CAP
    blocks = gate_weight.shape[0] // local
    hidden_here = gate_weight.shape[2]
    piece = model // 2 // TURNS
    anywhere = pl.BlockSpec(memory_space=pl.ANY)
    vmem = pltpu.VMEM
    weight = (gate_weight.shape[0], hidden_here, model)
    hidden, expert_out = pl.pallas_call(
        functools.partial(layer_kernel, count),
        out_shape=(shape((tokens, model // 2), bf16), shape((tokens, model // 2), bf16)),
        in_specs=[anywhere] * 13,
        out_specs=(anywhere, anywhere),
        scratch_shapes=[
            vmem((TOPK, tokens), jnp.int32),
            vmem((1, tokens), jnp.int32),
            vmem((1, tokens), jnp.int32),
            vmem((1, model), f32),
            vmem((tokens * heads, columns), bf16),
            vmem((2, requests, columns, positions), bf16),
            vmem((heads, count) + value_proj.shape[1:], bf16),
            vmem(out_proj.shape, bf16),
            vmem((tokens, model), bf16),
            vmem((count, tokens, width // 2), bf16),
            vmem((EXPERTS, model), bf16),
            vmem(weight, bf16),
            vmem(weight, bf16),
            vmem(weight, bf16),
            vmem((tokens * heads, 128), f32),
            vmem((LATENT // 128, tokens * heads, 128), f32),
            vmem((tokens, heads * VDIM), bf16),
            vmem((count, tokens, heads * VDIM), bf16),
            vmem((count, tokens, width // 2), f32),
            vmem((count, count, 2, tokens, width // 2), bf16),
            vmem((count, 8, 128), jnp.int32),
            vmem((8, count * tokens), jnp.int32),
            vmem((count, local * CAP, tokens), bf16),
            vmem((EXPERTS, count * tokens), f32),
            vmem((local, slots), f32),
            vmem((local, 2 * blocks * hidden_here, slots), f32),
            vmem((count, tokens, local * CAP), bf16),
            vmem((local, slots, blocks * hidden_here), bf16),
            vmem((TURNS, tokens, count * piece), bf16),
            vmem((TURNS, far * tokens, piece), bf16),
            vmem((TURNS, far - 1, tokens, piece), bf16),
            dma(10), dma(), dma(), dma(2), dma(2), dma(2),
            dma(), dma(2, far, PARTS), dma(), dma(2, far, PARTS), dma(), dma(count),
            dma(), dma(count, 2, far), dma(), dma(count),
            dma(), dma(TURNS), dma(), dma(TURNS), dma(), dma(TURNS), dma(2),
        ],
        compiler_params=pltpu.CompilerParams(
            collective_id=0, has_side_effects=True, vmem_limit_bytes=56 * 2**20
        ),
    )(
        expert_ids.T, token_visible[None], token_request[None], norm_gain[None], queries.reshape(tokens * heads, columns),
        jnp.swapaxes(latent_cache, 1, 2), value_proj, out_proj, residual, router.T,
        jnp.swapaxes(gate_weight, 1, 2), jnp.swapaxes(up_weight, 1, 2), down_weight,
    )
    half_block = vmem((tokens, model // 2), bf16)
    return pl.pallas_call(
        store_kernel,
        out_shape=(shape((tokens, model // 2), bf16), shape((tokens, model // 2), bf16)),
        in_specs=[anywhere] * 2,
        out_specs=(anywhere, anywhere),
        scratch_shapes=[half_block, half_block, dma(2), dma(2)],
        compiler_params=pltpu.CompilerParams(vmem_limit_bytes=56 * 2**20),
    )(hidden, expert_out)


LEAN_BYTES = 8 * 2**20


def choose(mesh):
    count = mesh.shape["ep"]

    def layer(*args):
        tokens, model = args[2].shape
        fits = count * tokens * model * 2 <= LEAN_BYTES
        even = count % 2 == 0 and count >= 4 and tokens % 32 == 0 and EXPERTS % count == 0
        if fits and even and mesh.shape["tp"] == 2:
            return lean_body(*args)
        return body(*args)

    return layer


def solution(mesh):
    return jax.shard_map(
        choose(mesh),
        mesh=mesh,
        in_specs=(
            P(("grp", "ep"), "tp", None),
            P(("grp", "ep"), "tp", None),
            P(("grp", "ep"), None),
            P(("grp", "ep")),
            P(("grp", "ep")),
            P("tp", "ep", None),
            P("tp", "ep"),
            P(),
            P(),
            P(("grp", "ep"), None),
            P("ep", None, "tp"),
            P("ep", None, "tp"),
            P("ep", "tp", None),
        ),
        out_specs=(P(("grp", "ep"), "tp"), P(("grp", "ep"), "tp")),
        check_vma=False,
    )
```

```python
import functools

import jax
import jax.numpy as jnp
from jax import lax
from jax.experimental import pallas as pl
from jax.experimental.pallas import tpu as pltpu
from jax.sharding import PartitionSpec as P

LATENT = 512
VDIM = 128
EXPERTS = 64
TOPK = 6
GROUPS = 2
CAP = 8
PIECES = 128
MESH = pl.DeviceIdType.MESH


score_scale = 192.0 ** (-0.5)
epsilon = 1e-06


def masked_scores(queries, block_rows, token_request, token_visible):
    per_request = block_rows.shape[1]
    flat_rows = block_rows.reshape(-1, block_rows.shape[2])
    scores = (
        jnp.einsum("thc,kc->thk", queries, flat_rows, preferred_element_type=jnp.float32)
        * score_scale
    )
    column = jnp.arange(flat_rows.shape[0], dtype=jnp.int32)
    owner_id = column // per_request
    position = column % per_request
    allowed = (owner_id[None, :] == token_request[:, None]) & (
        position[None, :] < token_visible[:, None]
    )
    return (jnp.where(allowed[:, None, :], scores, -jnp.inf), flat_rows)


def weighted_rows(scores, row_peak, flat_rows):
    weights = jnp.exp(scores - row_peak[:, :, None]).astype(jnp.bfloat16)
    totals = jnp.sum(weights.astype(jnp.float32), axis=2)
    summed = jnp.einsum(
        "thk,kc->thc", weights, flat_rows[:, :LATENT], preferred_element_type=jnp.float32
    )
    return (summed, totals)


def expert_block(arrived, gate_weight, up_weight, down_weight):
    gate_vals = jnp.einsum("prd,pdf->prf", arrived, gate_weight, preferred_element_type=jnp.float32)
    up_vals = jnp.einsum("prd,pdf->prf", arrived, up_weight, preferred_element_type=jnp.float32)
    activated = (jax.nn.silu(gate_vals) * up_vals).astype(jnp.bfloat16)
    return jnp.einsum(
        "prf,pfd->prd", activated, down_weight, preferred_element_type=jnp.float32
    ).astype(jnp.bfloat16)


def body(
    queries,
    latent_cache,
    residual,
    token_request,
    token_visible,
    value_proj,
    out_proj,
    norm_gain,
    router,
    expert_ids,
    gate_weight,
    up_weight,
    down_weight,
):
    all_rows = lax.all_gather(latent_cache, "tp", axis=1, tiled=True)
    scores, flat_rows = masked_scores(queries, all_rows, token_request, token_visible)
    summed, totals = weighted_rows(scores, jnp.max(scores, axis=2), flat_rows)
    context = (summed / totals[:, :, None]).astype(jnp.bfloat16)
    tokens_here = context.shape[0]
    heads_here = context.shape[1]
    head_values = jnp.einsum(
        "thl,hlv->thv",
        context,
        lax.all_gather(value_proj, "ep", axis=1, tiled=True),
        preferred_element_type=jnp.float32,
    )
    heads_out = head_values.astype(jnp.bfloat16).reshape(tokens_here, heads_here * VDIM)
    column_block = jnp.dot(
        lax.all_gather(heads_out, "ep", axis=0, tiled=True),
        out_proj,
        preferred_element_type=jnp.float32,
    )
    attention_part = lax.all_to_all(column_block, "ep", split_axis=0, concat_axis=1, tiled=True)
    attention = lax.psum(attention_part, "tp")
    hidden = (residual.astype(jnp.float32) + attention).astype(jnp.bfloat16)
    hidden_wide = hidden.astype(jnp.float32)
    normed = (
        hidden_wide
        * lax.rsqrt(jnp.mean(hidden_wide * hidden_wide, axis=1, keepdims=True) + epsilon)
        * norm_gain
    ).astype(jnp.bfloat16)
    logits = jnp.dot(normed, router, preferred_element_type=jnp.float32)
    gate_share = jax.nn.softmax(jnp.take_along_axis(logits, expert_ids, axis=1), axis=1).astype(
        jnp.bfloat16
    )
    flat_ids = expert_ids.reshape(-1)
    position_id = jnp.arange(flat_ids.shape[0], dtype=jnp.int32)
    earlier = (flat_ids[:, None] == flat_ids[None, :]) & (
        position_id[None, :] < position_id[:, None]
    )
    slot_ids = (flat_ids * CAP + jnp.sum(earlier.astype(jnp.int32), axis=1)).reshape(
        tokens_here, TOPK
    )
    targets = jnp.arange(EXPERTS * CAP, dtype=jnp.int32)
    matches = slot_ids[:, :, None] == targets[None, None, :]
    picker = jnp.any(matches, axis=1).T.astype(jnp.bfloat16)
    model_width = normed.shape[1]
    mixing = jnp.sum(
        jnp.where(matches, gate_share[:, :, None], jnp.zeros((), jnp.bfloat16)), axis=1
    )
    mixing = jnp.broadcast_to(
        mixing.reshape(tokens_here, EXPERTS, 1, CAP), (tokens_here, EXPERTS, GROUPS, CAP)
    ).reshape(tokens_here, PIECES * CAP)
    core_count = lax.axis_size("tp")
    half_width = model_width // core_count
    core_start = lax.axis_index("tp") * half_width
    outgoing = jnp.dot(picker, normed, preferred_element_type=jnp.float32).astype(jnp.bfloat16)
    outgoing = jnp.broadcast_to(
        outgoing.reshape(EXPERTS, 1, CAP, model_width), (EXPERTS, GROUPS, CAP, model_width)
    ).reshape(PIECES, CAP, model_width)
    arrived = lax.all_to_all(outgoing, "ep", split_axis=0, concat_axis=1, tiled=True)
    partial_out = expert_block(arrived, gate_weight, up_weight, down_weight)
    returned = lax.all_to_all(partial_out, "ep", split_axis=1, concat_axis=0, tiled=True)
    routed = jnp.dot(
        mixing, returned.reshape(PIECES * CAP, model_width), preferred_element_type=jnp.float32
    )
    expert_out = lax.psum_scatter(
        routed.astype(jnp.bfloat16), "tp", scatter_dimension=1, tiled=True
    )
    hidden_part = lax.dynamic_slice_in_dim(hidden, core_start, half_width, 1)
    return (hidden_part, expert_out)


def ring_position(index, count):
    half = lax.div(index, 2)
    return half + lax.rem(index, 2) * (count - 1 - 2 * half)


def ring_index(place, count):
    place = lax.rem(place + count, count)
    upper = lax.div(place, count // 2)
    return 2 * place + upper * (2 * count - 1 - 4 * place)


def greet(count):
    me = lax.axis_index("ep")
    core = lax.axis_index("tp")
    barrier = pltpu.get_barrier_semaphore()
    for step in range(1, count):
        pl.semaphore_signal(
            barrier, inc=1, device_id={"ep": lax.rem(me + step, count)}, device_id_type=MESH
        )
    pl.semaphore_signal(barrier, inc=1, device_id={"tp": 1 - core}, device_id_type=MESH)
    pl.semaphore_wait(barrier, count)


def remote(src, dst, send_sem, recv_sem, where):
    return pltpu.make_async_remote_copy(
        src_ref=src,
        dst_ref=dst,
        send_sem=send_sem,
        recv_sem=recv_sem,
        device_id=where,
        device_id_type=MESH,
    )


def drain(ref, sem):
    pltpu.make_async_copy(ref, ref, sem).wait()


def copy_here(src, dst, sem):
    copy = pltpu.make_async_copy(src, dst, sem)
    copy.start()
    return copy


class Ring:
    def __init__(self, count, own, slot, send_sem, recv_sem):
        self.count = count
        self.place = ring_position(lax.axis_index("ep"), count)
        self.far = count // 2
        self.near = count - 1 - self.far
        self.to = (ring_index(self.place + 1, count), ring_index(self.place - 1, count))
        self.own, self.slot = own, slot
        self.send_sem, self.recv_sem = send_sem, recv_sem
        self.hops = {}
        self.order = [
            (way, part)
            for turn in range(2)
            for pair in range(PARTS // 2)
            for way in range(2)
            for part in (2 * pair + (way + turn) % 2,)
        ]

    def reach(self, way, part):
        return self.far if way == part % 2 else self.near

    def origin(self, way, step):
        return ring_index(self.place - step if way == 0 else self.place + step, self.count)

    def hop(self, way, step, part):
        if step > self.reach(way, part):
            return
        block = self.origin(way, step - 1)
        self.hops[way, step, part] = remote(
            self.own(part) if step == 1 else self.slot(block, part),
            self.slot(block, part),
            self.send_sem,
            self.recv_sem.at[way, step - 1, part],
            {"ep": self.to[way]},
        )
        self.hops[way, step, part].start()

    def launch(self):
        for way, part in self.order:
            self.hop(way, 1, part)

    def relay(self, step):
        for way, part in self.order:
            if step <= self.reach(way, part):
                self.hops[way, step, part].wait_recv()
                self.hop(way, step + 1, part)

def number_of(offset, count):
    far = count // 2
    offset = offset % count
    if offset > far:
        offset -= count
    if offset == 0:
        return 0
    if offset == far:
        return count - 1
    return -2 * offset - 1 if offset < 0 else 2 * offset


def offset_of(number, count):
    if number == count - 1:
        return count // 2
    step = (number + 1) // 2
    return -step if number % 2 else step


class Pieces:
    def __init__(self, count, held, ring_send, ring_recv, side_send, side_recv):
        self.count = count
        self.place = ring_position(lax.axis_index("ep"), count)
        self.core = lax.axis_index("tp")
        self.far = count // 2
        self.near = count - 1 - self.far
        self.to = (ring_index(self.place + 1, count), ring_index(self.place - 1, count))
        self.held = held
        self.sems = (ring_send, ring_recv, side_send, side_recv)
        self.hops, self.sides = {}, {}

    def piece(self, offset, number):
        block = ring_index(self.place + offset + offset_of(number, self.count), self.count)
        return self.held.at[block, ring_index(self.place + offset, self.count), self.core]

    def reach(self, way, number):
        return self.far if number % 2 == way else self.near

    def hop(self, way, step, number):
        if step > self.reach(way, number):
            return
        ref = self.piece(-(step - 1) if way == 0 else step - 1, number)
        copy = remote(
            ref, ref, self.sems[0], self.sems[1].at[number, way, step - 1], {"ep": self.to[way]}
        )
        copy.start()
        self.hops[way, step, number] = copy

    def side(self, offset, number):
        ref = self.piece(offset, number)
        remote(ref, ref, self.sems[2], self.sems[3].at[offset % self.count], {"tp": 1 - self.core}).start()

    def launch(self, number):
        for turn in range(2):
            self.hop((number + turn) % 2, 1, number)
        self.side(0, number)

    def relay(self, step, number):
        for turn in range(2):
            way = (number + turn) % 2
            if step <= self.reach(way, number):
                self.hops[way, step, number].wait_recv()
                self.hop(way, step + 1, number)
                self.side(-step if way == 0 else step, number)

    def settle(self, offset):
        drain(self.held.at[0, :, 0], self.sems[3].at[offset % self.count])

    def finish(self):
        drain(self.held.at[: self.count - 1, :, 0], self.sems[0])
        drain(self.held.at[:, :, 0], self.sems[2])


def group_of(step, count):
    far = count // 2
    if step == 0:
        return [0]
    if step == far:
        return [count - 1]
    return [2 * step - 1, 2 * step]


ROWS = 256
PARTS = 4


def layer_kernel(
    count, ids_hbm, visible_hbm, request_hbm, gain_hbm, queries_hbm, cache_hbm, value_hbm, proj_hbm, residual_hbm, router_hbm,
    gate_hbm, up_hbm, down_hbm, hidden_hbm, out_hbm,
    ids_ref, visible_ref, request_ref, gain_ref,
    queries, cache, values, proj, residual_own, residual, router, gate, up, down,
    limits, context, heads_own, heads_all, theirs, held, ids_all, ids_row, hits, logits_v, scales, excited, mixing, active,
    sums2, inbox, inbox2,
    load_sem, excite_sem, lower_sem, swap_sem, id_sem, res_sem,
    value_send, value_recv, heads_send, heads_recv, pair_send, pair_recv,
    piece_send, piece_recv, side_send, side_recv,
    both_send, both_recv, cross_send, cross_recv, back_send, back_recv, store_sem,
):
    me = lax.axis_index("ep")
    core = lax.axis_index("tp")
    f32, bf16 = jnp.float32, jnp.bfloat16
    heads, _, latent, vdim = values.shape[0], values.shape[1], values.shape[1] * values.shape[2], values.shape[3]
    tokens = heads_own.shape[0]
    model = residual_own.shape[1]
    width = proj.shape[1]
    part = width // 2
    requests, columns, positions = cache.shape[1:]
    local = EXPERTS // count
    blocks = gate.shape[0] // local
    some = heads // PARTS
    half = tokens // PARTS
    place = ring_position(me, count)
    far = count // 2

    load_value = copy_here(value_hbm, values.at[:, me], load_sem.at[0])
    load_cache = copy_here(cache_hbm, cache.at[core], load_sem.at[1])
    load_small = [
        copy_here(source, target, load_sem.at[6 + number])
        for number, (source, target) in enumerate(
            ((ids_hbm, ids_ref), (visible_hbm, visible_ref), (request_hbm, request_ref), (gain_hbm, gain_ref))
        )
    ]
    load_residual = copy_here(residual_hbm, residual_own, load_sem.at[2])
    load_queries = copy_here(queries_hbm, queries, load_sem.at[3])
    load_proj = copy_here(proj_hbm, proj, load_sem.at[4])
    load_router = copy_here(router_hbm, router, load_sem.at[5])
    greet(count)

    load_value.wait()
    value_ring = Ring(
        count,
        lambda p: values.at[pl.ds(p * some, some), me],
        lambda block, p: values.at[pl.ds(p * some, some), block],
        value_send, value_recv,
    )
    value_ring.launch()
    for copy in load_small:
        copy.wait()
    ids_all[me, :TOPK, :tokens] = ids_ref[...]
    load_cache.wait()
    swap = remote(cache.at[core], cache.at[core], swap_sem.at[0], swap_sem.at[1], {"tp": 1 - core})
    swap.start()
    load_residual.wait()
    load_queries.wait()
    load_proj.wait()
    load_router.wait()
    for expert in range(local):
        span = pl.ds(expert * blocks, blocks)
        for source, target in ((gate_hbm, gate), (up_hbm, up)):
            pltpu.make_async_copy(source.at[span], target.at[span], excite_sem).start()
    load_down = copy_here(down_hbm, down, lower_sem)
    spreads = []
    for step in range(1, count):
        peer = lax.rem(me + step, count)
        column = pl.multiple_of(peer * width + core * part, part)
        spreads.append(
            remote(residual_own.at[:, pl.ds(column, part)], residual.at[me], res_sem.at[0], res_sem.at[1], {"ep": peer})
        )
        spreads.append(remote(ids_all.at[me], ids_all.at[me], id_sem.at[0], id_sem.at[1], {"ep": peer}))
    residual[me] = residual_own[:, pl.ds(pl.multiple_of(me * width + core * part, part), part)]

    visible, request = visible_ref[...], request_ref[...]
    row_token = lax.broadcasted_iota(jnp.int32, (tokens * heads, tokens), 0) // heads
    own_token = row_token == lax.broadcasted_iota(jnp.int32, (tokens * heads, tokens), 1)
    for r in range(requests):
        seen = jnp.where(request == r, visible, 0).astype(f32)
        limits[:, r : r + 1] = jnp.sum(jnp.where(own_token, seen, 0.0), axis=1, keepdims=True)

    def attend(start):
        rows = pl.ds(start, ROWS)
        asked = queries[rows, :]
        lane = lax.broadcasted_iota(jnp.int32, (ROWS, positions), 1).astype(f32)
        scored = []
        peak = None
        for r in range(requests):
            limit = limits[rows, r : r + 1]
            for side in range(2):
                score = jnp.dot(asked, cache[side, r], preferred_element_type=f32) * score_scale
                score = jnp.where(lane + float(side * positions) < limit, score, -jnp.inf)
                scored.append(score)
                top = jnp.max(score, axis=1, keepdims=True)
                peak = top if peak is None else jnp.maximum(peak, top)
        total, summed = None, None
        for number, score in enumerate(scored):
            weight = jnp.exp(score - peak).astype(bf16)
            amount = jnp.sum(weight.astype(f32), axis=1, keepdims=True)
            r, side = number // 2, number % 2
            term = lax.dot_general(
                weight, cache[side, r, :latent, :], (((1,), (1,)), ((), ())), preferred_element_type=f32
            )
            total = amount if total is None else total + amount
            summed = term if summed is None else summed + term
        summed = summed / total
        for piece in range(latent // 128):
            context[piece, rows, :] = summed[:, piece * 128 : (piece + 1) * 128]

    swap.wait_recv()
    chunks = list(range(0, tokens * heads, ROWS))
    for step in range(1, far + 1):
        if chunks:
            attend(chunks.pop(0))
        value_ring.relay(step)
        if step == 3:
            for copy in spreads:
                copy.start()
    for start in chunks:
        attend(start)
    for h in range(heads):
        rows = jnp.concatenate(
            [context[piece, pl.ds(h, tokens, stride=heads), :] for piece in range(latent // 128)], axis=1
        ).astype(bf16)
        heads_own[:, h * vdim : (h + 1) * vdim] = jnp.dot(
            rows, values[h].reshape(latent, vdim), preferred_element_type=f32
        ).astype(bf16)

    heads_ring = Ring(
        count,
        lambda p: heads_own.at[pl.ds(p * half, half)],
        lambda block, p: heads_all.at[block, pl.ds(p * half, half)],
        heads_send, heads_recv,
    )
    heads_ring.launch()
    mine = context
    pieces = Pieces(count, held, piece_send, piece_recv, side_send, side_recv)
    pairs = {}

    def block_at(offset):
        return ring_index(place + offset, count)

    def project(number):
        rows = heads_own[...] if number == 0 else heads_all[block_at(offset_of(number, count))]
        product = jnp.dot(rows, proj[...], preferred_element_type=f32)
        rows = pl.ds(number * tokens, tokens)
        mine[0, rows, :] = product[:, :part]
        mine[1, rows, :] = product[:, part:]
        copy = remote(
            mine.at[1 - core, rows, :], theirs.at[number], pair_send, pair_recv.at[number],
            {"tp": 1 - core},
        )
        copy.start()
        pairs[number] = copy

    def conclude(number):
        if number == 0:
            drain(residual.at[: count - 1], res_sem.at[1])
            drain(ids_all.at[: count - 1], id_sem.at[1])
        pairs[number].wait_recv()
        block = block_at(offset_of(number, count))
        attention = mine[core, pl.ds(number * tokens, tokens), :] + theirs[number]
        held[block, me, core] = (residual[block].astype(f32) + attention).astype(bf16)
        pieces.launch(number)

    squares = limits
    around = [offset if offset <= far else offset - count for offset in range(count)]
    dims = (((1,), (1,)), ((), ()))
    inner = blocks * gate.shape[1]

    def place_slots():
        before = (
            lax.broadcasted_iota(jnp.int32, (tokens, tokens), 0)
            < lax.broadcasted_iota(jnp.int32, (tokens, tokens), 1)
        ).astype(bf16)
        ids = [ids_all[block_at(offset)][:, :tokens] for offset in around]
        ids_row[...] = jnp.concatenate(ids, axis=1)
        expert = lax.broadcasted_iota(jnp.int32, (local, tokens), 0) + me * local
        here = []
        for one in ids:
            named = expert == one[0:1]
            for k in range(1, TOPK):
                named = named | (expert == one[k : k + 1])
            here.append(named.astype(f32))
        here = jnp.concatenate(here, axis=0)
        rank = jnp.dot(here.astype(bf16), before, preferred_element_type=f32)
        slot = lax.broadcasted_iota(jnp.int32, (count * local, CAP, tokens), 1).astype(f32)
        hit = (here[:, None, :] > 0.5) & (rank[:, None, :] == slot)
        hits[...] = jnp.where(hit, 1.0, 0.0).reshape(count, local * CAP, tokens).astype(bf16)

    def columns_of(offset):
        return pl.ds(pl.multiple_of(block_at(offset) * width, width), width)

    def prepare(offset):
        owner = block_at(offset)
        gain = gain_ref[:, columns_of(offset)]
        first = offset == 0
        scaled, chosen = [], []
        for index, other in enumerate(around):
            span = pl.ds(index * tokens, tokens)
            block = block_at(other)
            sides = [held[block, owner, c].astype(f32) for c in range(2)]
            square = sides[0] * sides[0] + sides[1] * sides[1]
            squares[span, :] = square if first else squares[span, :] + square
            wide = (jnp.concatenate(sides, axis=1) * gain).astype(bf16)
            scaled.append(wide)
            chosen.append(jnp.dot(hits[index], wide, preferred_element_type=f32))
        part_logits = lax.dot_general(
            router[:, columns_of(offset)], jnp.concatenate(scaled, axis=0), dims, preferred_element_type=f32
        )
        logits_v[...] = part_logits if first else logits_v[...] + part_logits
        return [
            jnp.concatenate(
                [one[expert * CAP : (expert + 1) * CAP] for one in chosen], axis=0
            ).astype(bf16)
            for expert in range(local)
        ]

    def stream(offset, slots):
        column = columns_of(offset)
        for expert in range(local):
            span = pl.ds(expert * blocks, blocks)
            weights = jnp.concatenate(
                [weight[span, :, column].reshape(inner, width) for weight in (gate, up)], axis=0
            )
            term = lax.dot_general(weights, slots[expert], dims, preferred_element_type=f32)
            excited[expert] = term if offset == 0 else excited[expert] + term

    def contract(offset, last=False):
        pieces.settle(offset)
        slots = prepare(offset)
        if last:
            weigh()
        stream(offset, slots)

    def weigh():
        mean = jnp.sum(squares[...], axis=1, keepdims=True) / model
        scale = jnp.broadcast_to(lax.rsqrt(mean + epsilon), squares.shape).T[:1]
        lane = lax.broadcasted_iota(jnp.int32, (count * CAP, 128), 1)
        slot_scale = jnp.zeros((count * CAP, 128), f32)
        slot_scales = [
            jnp.sum(hits[index].astype(f32) * scale[:, index * tokens : (index + 1) * tokens], axis=1, keepdims=True)
            for index in range(count)
        ]
        for expert in range(local):
            own = jnp.concatenate([one[expert * CAP : (expert + 1) * CAP] for one in slot_scales], axis=0)
            slot_scale = jnp.where(lane == expert, own, slot_scale)
        scales[...] = slot_scale.T[:local]
        expert_row = lax.broadcasted_iota(jnp.int32, (EXPERTS, count * tokens), 0)
        named = expert_row == ids_row[0:1, :]
        for k in range(1, TOPK):
            named = named | (expert_row == ids_row[k : k + 1, :])
        logits = jnp.where(named, logits_v[...] * scale, -jnp.inf)
        raised = jnp.exp(logits - jnp.max(logits, axis=0, keepdims=True))
        logits_v[...] = raised / jnp.sum(raised, axis=0, keepdims=True)
        share = logits_v[pl.ds(pl.multiple_of(me * local, local), local), :].astype(bf16).astype(f32)
        for index in range(count):
            own = share[:, None, index * tokens : (index + 1) * tokens]
            own = jnp.broadcast_to(own, (local, CAP, tokens)).reshape(local * CAP, tokens)
            mixing[index] = (hits[index].astype(f32) * own).T.astype(bf16)

    def activate():
        for expert in range(local):
            row = scales[expert : expert + 1]
            gate_t = excited[expert, :inner, :] * row
            up_t = excited[expert, inner:, :] * row
            active[expert] = (gate_t / (1.0 + jnp.exp(-gate_t)) * up_t).T.astype(bf16)

    due = {far: [0], far + 1: [1]}
    for distance in range(2, far):
        due[far + distance] = [1 - distance, distance]
    due[2 * far] = [1 - far, far]
    for turn in range(2 * far + 1):
        if turn == far:
            drain(gate, excite_sem)
            drain(up, excite_sem)
        if 1 <= turn <= far:
            heads_ring.relay(turn)
        if turn <= far:
            for number in group_of(turn, count):
                project(number)
        for group in range(far + 1):
            if 1 <= turn - group <= far:
                for number in group_of(group, count):
                    pieces.relay(turn - group, number)
        if turn <= far:
            for number in group_of(turn, count):
                conclude(number)
        if turn == 0:
            place_slots()
        for offset in due.get(turn, ()):
            contract(offset, offset == far)
    activate()

    for e in range(count // 2):
        for c in range(2):
            number = 2 * e + c
            copy_here(
                held.at[me, (count // 2) * core + e, c],
                hidden_hbm.at[:, pl.ds(number * part, part)],
                store_sem.at[0],
            )
    load_down.wait()

    turns = sums2.shape[0]
    piece = sums2.shape[2] // count
    sums = gate
    side_width = model // 2
    twin = me + 1 - 2 * lax.rem(me, 2)
    pair = count // 2
    steps = list(range(1, pair)) + [0]
    near_order = [lax.rem(me + 2 * step, count) for step in steps]
    twin_order = [lax.rem(twin + 2 * step, count) for step in steps]
    boths, crosses = {}, {}

    def lanes_of(block):
        return pl.ds(pl.multiple_of(block * piece, piece), piece)

    def lower(turn):
        rows = []
        for expert in range(local):
            span = pl.ds(expert * blocks, blocks)
            sides = [
                jnp.dot(
                    active[expert],
                    down[span, :, pl.ds(c * side_width + turn * piece, piece)].reshape(inner, piece),
                    preferred_element_type=f32,
                )
                for c in range(2)
            ]
            rows.append(jnp.concatenate(sides, axis=1))
        for offset in range(count):
            mine_rows = [row[offset * CAP : (offset + 1) * CAP] for row in rows]
            mixed = jnp.dot(
                mixing[offset], jnp.concatenate(mine_rows, axis=0).astype(bf16), preferred_element_type=f32
            ).astype(bf16)
            for c in range(2):
                sums[2 * turn + c, :tokens, lanes_of(block_at(offset))] = mixed[:, c * piece : (c + 1) * piece]
        boths[turn] = remote(
            sums.at[2 * turn + 1 - core, pl.ds(0, tokens), pl.ds(0, count * piece)], sums2.at[turn], both_send, both_recv.at[turn],
            {"tp": 1 - core},
        )
        boths[turn].start()

    def added(turn, block):
        own = sums[2 * turn + core, :tokens, lanes_of(block)]
        return own.astype(f32) + sums2[turn, :, lanes_of(block)].astype(f32)

    swap.wait_send()
    fits = columns // (pair * tokens)

    def outbox(which, turn, rows):
        at, lane = turn // (positions // piece), turn % (positions // piece)
        return cache.at[
            which, at // fits, pl.ds(at % fits * pair * tokens, rows), pl.ds(lane * piece, piece)
        ]

    def cross(turn):
        boths[turn].wait_recv()
        box = outbox(0, turn, pair * tokens)
        for i, block in enumerate(twin_order):
            box[i * tokens : (i + 1) * tokens, :] = added(turn, block).astype(bf16)
        crosses[turn] = remote(box, inbox.at[turn], cross_send, cross_recv.at[turn], {"ep": twin})
        crosses[turn].start()

    def back(turn):
        crosses[turn].wait_recv()
        box = outbox(1, turn, (pair - 1) * tokens)
        for i, block in enumerate(near_order):
            rows = pl.ds(i * tokens, tokens)
            total = added(turn, block) + inbox[turn, rows, :].astype(f32)
            if i == pair - 1:
                limits[turn * tokens : (turn + 1) * tokens, :piece] = total
                continue
            box[rows, :] = total.astype(bf16)
            remote(box.at[rows, :], inbox2.at[turn, i], back_send, back_recv.at[turn], {"ep": block}).start()

    def end(turn):
        total = limits[turn * tokens : (turn + 1) * tokens, :piece]
        drain(inbox2.at[turn], back_recv.at[turn])
        for i in range(pair - 1):
            total = total + inbox2[turn, i].astype(f32)
        span = pl.ds(turn * piece, piece)
        out_v[:, span] = total.astype(bf16)
        copy_here(out_v.at[:, span], out_hbm.at[:, span], store_sem.at[1])

    for turn in range(turns + 3):
        if turn < turns:
            lower(turn)
        if 1 <= turn <= turns:
            cross(turn - 1)
        if turn >= 3:
            back(turn - 3)
    drain(heads_all.at[: count - 1], heads_send)
    out_v = heads_own
    for turn in range(turns):
        end(turn)

    drain(values.at[:, : count - 1], value_send)
    pieces.finish()
    drain(residual.at[: count - 1], res_sem.at[0])
    drain(ids_all.at[: count - 1], id_sem.at[0])
    drain(theirs, pair_send)
    drain(sums2, both_send)
    drain(inbox, cross_send)
    drain(inbox2, back_send)
    drain(heads_own, store_sem.at[0])
    drain(heads_own, store_sem.at[1])


def store_kernel(hidden_hbm, out_hbm, hidden_to, out_to, hidden_v, out_v, in_sem, out_sem):
    loads = [copy_here(hidden_hbm, hidden_v, in_sem.at[0]), copy_here(out_hbm, out_v, in_sem.at[1])]
    loads[0].wait()
    stores = [copy_here(hidden_v, hidden_to, out_sem.at[0])]
    loads[1].wait()
    stores.append(copy_here(out_v, out_to, out_sem.at[1]))
    for copy in stores:
        copy.wait()


def dma(*shape):
    return pltpu.SemaphoreType.DMA(shape)


TURNS = 8


def lean_body(
    queries,
    latent_cache,
    residual,
    token_request,
    token_visible,
    value_proj,
    out_proj,
    norm_gain,
    router,
    expert_ids,
    gate_weight,
    up_weight,
    down_weight,
):
    count = lax.axis_size("ep")
    tokens, heads, columns = queries.shape
    requests, positions, _ = latent_cache.shape
    model = residual.shape[1]
    bf16, f32 = jnp.bfloat16, jnp.float32
    shape = jax.ShapeDtypeStruct
    far = count // 2
    local = EXPERTS // count
    width = out_proj.shape[1]
    slots = count * CAP
    blocks = gate_weight.shape[0] // local
    hidden_here = gate_weight.shape[2]
    piece = model // 2 // TURNS
    anywhere = pl.BlockSpec(memory_space=pl.ANY)
    vmem = pltpu.VMEM
    weight = (gate_weight.shape[0], hidden_here, model)
    hidden, expert_out = pl.pallas_call(
        functools.partial(layer_kernel, count),
        out_shape=(shape((tokens, model // 2), bf16), shape((tokens, model // 2), bf16)),
        in_specs=[anywhere] * 13,
        out_specs=(anywhere, anywhere),
        scratch_shapes=[
            vmem((TOPK, tokens), jnp.int32),
            vmem((1, tokens), jnp.int32),
            vmem((1, tokens), jnp.int32),
            vmem((1, model), f32),
            vmem((tokens * heads, columns), bf16),
            vmem((2, requests, columns, positions), bf16),
            vmem((heads, count) + value_proj.shape[1:], bf16),
            vmem(out_proj.shape, bf16),
            vmem((tokens, model), bf16),
            vmem((count, tokens, width // 2), bf16),
            vmem((EXPERTS, model), bf16),
            vmem(weight, bf16),
            vmem(weight, bf16),
            vmem(weight, bf16),
            vmem((tokens * heads, 128), f32),
            vmem((LATENT // 128, tokens * heads, 128), f32),
            vmem((tokens, heads * VDIM), bf16),
            vmem((count, tokens, heads * VDIM), bf16),
            vmem((count, tokens, width // 2), f32),
            vmem((count, count, 2, tokens, width // 2), bf16),
            vmem((count, 8, 128), jnp.int32),
            vmem((8, count * tokens), jnp.int32),
            vmem((count, local * CAP, tokens), bf16),
            vmem((EXPERTS, count * tokens), f32),
            vmem((local, slots), f32),
            vmem((local, 2 * blocks * hidden_here, slots), f32),
            vmem((count, tokens, local * CAP), bf16),
            vmem((local, slots, blocks * hidden_here), bf16),
            vmem((TURNS, tokens, count * piece), bf16),
            vmem((TURNS, far * tokens, piece), bf16),
            vmem((TURNS, far - 1, tokens, piece), bf16),
            dma(10), dma(), dma(), dma(2), dma(2), dma(2),
            dma(), dma(2, far, PARTS), dma(), dma(2, far, PARTS), dma(), dma(count),
            dma(), dma(count, 2, far), dma(), dma(count),
            dma(), dma(TURNS), dma(), dma(TURNS), dma(), dma(TURNS), dma(2),
        ],
        compiler_params=pltpu.CompilerParams(
            collective_id=0, has_side_effects=True, vmem_limit_bytes=56 * 2**20
        ),
    )(
        expert_ids.T, token_visible[None], token_request[None], norm_gain[None], queries.reshape(tokens * heads, columns),
        jnp.swapaxes(latent_cache, 1, 2), value_proj, out_proj, residual, router.T,
        jnp.swapaxes(gate_weight, 1, 2), jnp.swapaxes(up_weight, 1, 2), down_weight,
    )
    half_block = vmem((tokens, model // 2), bf16)
    return pl.pallas_call(
        store_kernel,
        out_shape=(shape((tokens, model // 2), bf16), shape((tokens, model // 2), bf16)),
        in_specs=[anywhere] * 2,
        out_specs=(anywhere, anywhere),
        scratch_shapes=[half_block, half_block, dma(2), dma(2)],
        compiler_params=pltpu.CompilerParams(vmem_limit_bytes=56 * 2**20),
    )(hidden, expert_out)


LEAN_BYTES = 8 * 2**20


def choose(mesh):
    count = mesh.shape["ep"]

    def layer(*args):
        tokens, model = args[2].shape
        fits = count * tokens * model * 2 <= LEAN_BYTES
        even = count % 2 == 0 and count >= 4 and tokens % 32 == 0 and EXPERTS % count == 0
        if fits and even and mesh.shape["tp"] == 2:
            return lean_body(*args)
        return body(*args)

    return layer


def solution(mesh):
    return jax.shard_map(
        choose(mesh),
        mesh=mesh,
        in_specs=(
            P(("grp", "ep"), "tp", None),
            P(("grp", "ep"), "tp", None),
            P(("grp", "ep"), None),
            P(("grp", "ep")),
            P(("grp", "ep")),
            P("tp", "ep", None),
            P("tp", "ep"),
            P(),
            P(),
            P(("grp", "ep"), None),
            P("ep", None, "tp"),
            P("ep", None, "tp"),
            P("ep", "tp", None),
        ),
        out_specs=(P(("grp", "ep"), "tp"), P(("grp", "ep"), "tp")),
        check_vma=False,
    )
```
